32 devices in a mesh: section: 2 (over core), expert: 16 (over z, y, x).
Axes of the slice: x: 2, y: 2, z: 4, core: 2. Of those that a mesh axis runs over, the one named last changes fastest.
Arguments:
- act_in: bfloat16 [2, 2048, 7168], P('section', 'expert'), may hold values from -6 to 6
- cotangent: bfloat16 [2, 2048, 7168], P('section', 'expert'), may hold values from -6 to 6
- fwd_ids: int32 [2, 2048, 8], P('section', 'expert'), may hold values from 0 to 255, as said below
- fwd_gates: float32 [2, 2048, 8], P('section', 'expert'), may hold values from 0.05 to 0.8
- bwd_ids: int32 [2, 2048, 8], P('section', 'expert'), may hold values from 0 to 255, as said below
- bwd_gates: float32 [2, 2048, 8], P('section', 'expert'), may hold values from 0.05 to 0.8
- gate_w: bfloat16 [2, 7168, 2048], P('section', None, 'expert'), may hold values from -0.0625 to 0.0625
- up_w: bfloat16 [2, 7168, 2048], P('section', None, 'expert'), may hold values from -0.0625 to 0.0625
- down_w: bfloat16 [2, 2048, 7168], P('section', 'expert'), may hold values from -0.125 to 0.125
- gate_pre: bfloat16 [2, 160, 2048], P('section', None, 'expert'), may hold values from -6 to 6
- up_pre: bfloat16 [2, 160, 2048], P('section', None, 'expert'), may hold values from -6 to 6
Outputs:
- next_act: bfloat16 [2, 2048, 7168], P('section', 'expert')
- prev_grad: bfloat16 [2, 2048, 7168], P('section', 'expert')
- gate_grad: float32 [2, 2048, 8], P('section', 'expert')
The draws below stay inside these ranges and needn't reach their ends.
Inputs may be any that keep to these rules, and one draw needn't show every extreme that they name: `fwd_ids`: the 8 ids of a row differ. In each aligned block of 128 rows (the rows of one device) each id below 1 is named by at most 10 rows; in every section one such id is named by exactly 10 rows in every block. `bwd_ids`: as for fwd_ids.
All inputs are finite; a program needn't handle non-finite values.
Results may differ from the reference program's by a relative error of at most 0.012.
Values may be sent and summed in bfloat16 or wider, within the bound.
A program may use at most 128 MiB of HBM per device.

```python
import math
import jax
import jax.numpy as jnp
from jax import lax

D = 7168
FF = 2048
ROUTED = 256
TOP = 8
TOK_DEV = 128
CAP = 10
SLICES = 16
FF_DEV = 128
EXPERTS = 1
SECTIONS = 2
TOKENS = 2048
SLOTS = 160


def route_draw(key):
    blocks = SECTIONS * (TOKENS // TOK_DEV)
    keys = [jax.random.fold_in(key, offset) for offset in range(5)]
    counts = jax.random.randint(keys[0], (blocks, EXPERTS), CAP // 2, CAP + 1)
    fullest = jax.random.randint(keys[1], (SECTIONS,), 0, EXPERTS)
    fullest_block = jnp.repeat(fullest, TOKENS // TOK_DEV)
    counts = jnp.where(jnp.arange(EXPERTS)[None, :] == fullest_block[:, None], CAP, counts)
    scores = jax.random.randint(keys[2], (blocks, EXPERTS, TOK_DEV), 0, 2 ** 20) * TOK_DEV + jnp.arange(TOK_DEV)
    order = jnp.argsort(jnp.argsort(scores, axis=-1), axis=-1)
    chosen = order < counts[:, :, None]
    others = jax.random.randint(keys[3], (blocks, TOK_DEV, ROUTED - EXPERTS), 0, 2 ** 20) * ROUTED + jnp.arange(ROUTED - EXPERTS)
    unused, picks = lax.top_k(others, TOP)
    ids = picks + EXPERTS
    slot_scores = jax.random.randint(keys[4], (blocks, TOK_DEV, TOP), 0, 2 ** 20) * TOP + jnp.arange(TOP)
    unused_two, places = lax.top_k(slot_scores, TOP)
    slot_iota = jnp.arange(TOP)
    for expert in range(EXPERTS):
        target = places[:, :, expert:expert + 1]
        put_here = (slot_iota[None, None, :] == target) & chosen[:, expert, :, None]
        ids = jnp.where(put_here, expert, ids)
    return ids.reshape(SECTIONS, TOKENS, TOP).astype(jnp.int32)


def draw_fwd_ids(key, part):
    return route_draw(jax.random.fold_in(key, 11))


def draw_bwd_ids(key, part):
    return route_draw(jax.random.fold_in(key, 23))


def block_scale(key, extent, pieces, least, high):
    def one(dim, shards_of):
        draws = jax.random.uniform(jax.random.fold_in(jax.random.fold_in(key, 6), dim), (shards_of,), jnp.float32, least / len(pieces), high / len(pieces))
        return jnp.repeat(jnp.exp(draws), extent[dim] // shards_of).reshape((-1,) + (1,) * (len(extent) - dim - 1))

    level = one(*pieces[0])
    for cut in pieces[1:]:
        level = level * one(*cut)
    return level


def scatter_about(key, shape, width, reach, shards=(), held_as=jnp.bfloat16):
    values = width * jax.random.normal(key, shape, jnp.float32)
    if shards:
        values = values * block_scale(key, shape, shards, -0.22, 0.18)
    return jnp.clip(values, -reach, reach).astype(held_as)


def setup_inputs(seed: int = 0) -> dict:
    streams_of = jax.random.split(jax.random.key(seed), 12)
    return {
        "act_in": scatter_about(streams_of[0], (SECTIONS, TOKENS, D), 1.0, 6.0, ((0, 2), (1, 16))),
        "cotangent": scatter_about(streams_of[1], (SECTIONS, TOKENS, D), 1.0, 6.0, ((0, 2), (1, 16))),
        "fwd_ids": draw_fwd_ids(jax.random.fold_in(streams_of[11], 71), 0),
        "fwd_gates": jnp.clip(jnp.exp(math.log(0.8) - 2.7725887 * jax.random.uniform(streams_of[3], (SECTIONS, TOKENS, TOP), jnp.float32) ** block_scale(streams_of[3], (SECTIONS, TOKENS, TOP), ((0, 2), (1, 16)), -0.2, 0.2)), 0.05, 0.8),
        "bwd_ids": draw_bwd_ids(jax.random.fold_in(streams_of[11], 71), 0),
        "bwd_gates": jnp.clip(jnp.exp(math.log(0.8) - 2.7725887 * jax.random.uniform(streams_of[5], (SECTIONS, TOKENS, TOP), jnp.float32) ** block_scale(streams_of[5], (SECTIONS, TOKENS, TOP), ((0, 2), (1, 16)), -0.2, 0.2)), 0.05, 0.8),
        "gate_w": scatter_about(streams_of[6], (SECTIONS, D, EXPERTS * FF), D ** -0.5, 0.0625, ((0, 2), (2, 16))),
        "up_w": scatter_about(streams_of[7], (SECTIONS, D, EXPERTS * FF), D ** -0.5, 0.0625, ((0, 2), (2, 16))),
        "down_w": scatter_about(streams_of[8], (SECTIONS, EXPERTS * FF, D), FF ** -0.5, 0.125, ((0, 2), (1, 16))),
        "gate_pre": scatter_about(streams_of[9], (SECTIONS, SLOTS, EXPERTS * FF), 1.0, 6.0, ((0, 2), (2, 16))),
        "up_pre": scatter_about(streams_of[10], (SECTIONS, SLOTS, EXPERTS * FF), 1.0, 6.0, ((0, 2), (2, 16))),
    }


def slots_of(ids, expert):
    matches = ids == expert
    routed = jnp.any(matches, axis=1)
    blocks = routed.reshape(-1, TOK_DEV).astype(jnp.int32)
    position = (jnp.cumsum(blocks, axis=1) - 1).reshape(-1)
    block_ids = jnp.arange(TOKENS, dtype=jnp.int32) // TOK_DEV
    slot = jnp.where(routed, block_ids * CAP + position, SLOTS).astype(jnp.int32)
    return matches, slot


def place_rows(tokens, slot):
    empty = jnp.zeros((SLOTS, tokens.shape[1]), tokens.dtype)
    return empty.at[slot].set(tokens, mode="drop")


def take_rows(table, slot):
    return jnp.take(table, jnp.minimum(slot, SLOTS - 1).astype(jnp.int32), axis=0)


def rounded_sum(parts):
    rounded = lax.optimization_barrier(parts.astype(jnp.bfloat16))
    return jnp.sum(rounded.astype(jnp.float32), axis=0)


def section_layer(tokens, grads, ids_f, gates_f, ids_b, gates_b, w_gate, w_up, w_down, pre_gate, pre_up):
    mixed = jnp.zeros((TOKENS, D), jnp.float32)
    input_grad = jnp.zeros((TOKENS, D), jnp.float32)
    gate_grad = jnp.zeros((TOKENS, TOP), jnp.float32)
    for expert in range(EXPERTS):
        lo_col = expert * FF
        wg_e = w_gate[:, lo_col:lo_col + FF]
        wu_e = w_up[:, lo_col:lo_col + FF]
        wd_e = w_down[lo_col:lo_col + FF]
        matches, slot = slots_of(ids_f, expert)
        weights = jnp.sum(jnp.where(matches, gates_f, 0.0), axis=1)
        rows = place_rows(tokens, slot)
        gate_act = jnp.dot(rows, wg_e, preferred_element_type=jnp.float32)
        up_act = jnp.dot(rows, wu_e, preferred_element_type=jnp.float32)
        hidden = (jax.nn.silu(gate_act) * up_act).astype(jnp.bfloat16)
        parts = jnp.einsum("rsf,sfd->srd", hidden.reshape(SLOTS, SLICES, FF_DEV).astype(jnp.float32),
                           wd_e.reshape(SLICES, FF_DEV, D).astype(jnp.float32))
        expert_out = rounded_sum(parts)
        mixed = mixed + weights[:, None] * take_rows(expert_out, slot)

        matches_b, slot_b = slots_of(ids_b, expert)
        weights_b = jnp.sum(jnp.where(matches_b, gates_b, 0.0), axis=1)
        grad_rows = place_rows(grads, slot_b)
        saved_gate = pre_gate[:, lo_col:lo_col + FF].astype(jnp.float32)
        saved_up = pre_up[:, lo_col:lo_col + FF].astype(jnp.float32)
        grad_hidden = jnp.dot(grad_rows, wd_e.T, preferred_element_type=jnp.float32)
        sigmoid_gate = jax.nn.sigmoid(saved_gate)
        activated = saved_gate * sigmoid_gate
        dot_parts = jnp.sum((grad_hidden * activated * saved_up).reshape(SLOTS, SLICES, FF_DEV), axis=2)
        expert_dot = rounded_sum(dot_parts.T)
        grad_gate_act = (grad_hidden * saved_up * sigmoid_gate * (1.0 + saved_gate * (1.0 - sigmoid_gate))).astype(jnp.bfloat16)
        grad_up_act = (grad_hidden * activated).astype(jnp.bfloat16)
        grad_parts = jnp.einsum("rsf,dsf->srd", grad_gate_act.reshape(SLOTS, SLICES, FF_DEV).astype(jnp.float32),
                                wg_e.reshape(D, SLICES, FF_DEV).astype(jnp.float32))
        grad_parts = grad_parts + jnp.einsum("rsf,dsf->srd", grad_up_act.reshape(SLOTS, SLICES, FF_DEV).astype(jnp.float32),
                                             wu_e.reshape(D, SLICES, FF_DEV).astype(jnp.float32))
        expert_grad = rounded_sum(grad_parts)
        input_grad = input_grad + weights_b[:, None] * take_rows(expert_grad, slot_b)
        gate_grad = gate_grad + jnp.where(matches_b, take_rows(expert_dot, slot_b)[:, None], 0.0)
    return mixed.astype(jnp.bfloat16), input_grad.astype(jnp.bfloat16), gate_grad


def reference(act_in, cotangent, fwd_ids, fwd_gates, bwd_ids, bwd_gates, gate_w, up_w, down_w, gate_pre, up_pre):
    outputs = []
    grads = []
    gate_grads = []
    for section in range(SECTIONS):
        mixed, input_grad, gate_grad = section_layer(act_in[section], cotangent[section], fwd_ids[section], fwd_gates[section],
                                                   bwd_ids[section], bwd_gates[section], gate_w[section], up_w[section],
                                                   down_w[section], gate_pre[section], up_pre[section])
        outputs.append(mixed)
        grads.append(input_grad)
        gate_grads.append(gate_grad)
    next_act = jnp.roll(jnp.stack(outputs), 1, axis=0)
    prev_grad = jnp.roll(jnp.stack(grads), -1, axis=0)
    return next_act, prev_grad, jnp.stack(gate_grads)
```

```python
import functools
import math

import jax
import jax.numpy as jnp
from jax import lax
from jax.experimental import pallas as pl
from jax.experimental.pallas import tpu as pltpu
from jax.sharding import PartitionSpec as P

FF = 2048
QUAD = 4
LANES = 128
AHEAD = 3
SECOND_LAG = 1
THIRD_LAG = 2
SEMAPHORES = 128
MESH = pl.DeviceIdType.MESH


def from_behind(value, axis, steps):
    count = lax.axis_size(axis)
    pairs = [(source, (source + steps) % count) for source in range(count)]
    return lax.ppermute(value, axis, pairs)


def routing(ids, gates, experts, capacity):
    expert_ids = jnp.arange(experts, dtype=jnp.int32)
    matches = ids[None, :, :] == expert_ids[:, None, None]
    routed = jnp.any(matches, axis=2)
    weights = jnp.sum(jnp.where(matches, gates[None, :, :], 0.0), axis=2)
    tokens = ids.shape[0]
    earlier = jnp.arange(tokens)[:, None] <= jnp.arange(tokens)[None, :]
    counted = jnp.sum(jnp.where(routed[:, :, None] & earlier[None], 1, 0), axis=1)
    position = counted - 1
    slot_ids = jnp.arange(capacity, dtype=jnp.int32)
    placing = (position[:, None, :] == slot_ids[None, :, None]) & routed[:, None, :]
    return (matches, placing.astype(jnp.float32), weights)


def xor(value, mask):
    out = value
    bit = 1
    while bit <= mask:
        if mask & bit:
            out = out + bit - 2 * bit * ((value // bit) % 2)
        bit *= 2
    return out


def dot(a, b, dims=((1,), (0,))):
    return lax.dot_general(a, b, (dims, ((), ())), preferred_element_type=jnp.float32)


def wide(value):
    return value.astype(jnp.float32)


def narrow(value):
    return value.astype(jnp.bfloat16)


def padded(rows):
    return -(-rows // 16) * 16


def selection(count, rows, pad, flip=False):
    shape = (count * rows, count * pad) if flip else (count * pad, count * rows)
    long = lax.broadcasted_iota(jnp.int32, shape, 1 if flip else 0)
    short = lax.broadcasted_iota(jnp.int32, shape, 0 if flip else 1)
    piece = lax.shift_right_logical(long, jnp.int32(pad.bit_length() - 1))
    inner = long & (pad - 1)
    chosen = (short == piece * rows + inner) & (inner < rows)
    return narrow(jnp.where(chosen, 1.0, 0.0))


def slot_table(ids, rows):
    tokens = ids.shape[0]
    hit = jnp.where(ids == 0, 1.0, 0.0)
    routed = jnp.max(hit, axis=1, keepdims=True)
    spread = jnp.broadcast_to(routed, (tokens, LANES))
    row = lax.broadcasted_iota(jnp.int32, (tokens, tokens), 0)
    column = lax.broadcasted_iota(jnp.int32, (tokens, tokens), 1)
    lower = narrow(jnp.where(column <= row, 1.0, 0.0))
    rank = dot(lower, narrow(spread)) - 1.0
    lane = wide(lax.broadcasted_iota(jnp.int32, (tokens, LANES), 1))
    return jnp.where((rank == lane) & (spread > 0.0), 1.0, 0.0)


class Links:
    def __init__(self, send_sems, recv_sems):
        self.send_sems = send_sems
        self.recv_sems = recv_sems
        self.count = 0
        self.sent = []

    def copy(self, src, dst, peer, axis="expert"):
        k = self.count
        self.count += 1
        assert k < SEMAPHORES
        return pltpu.make_async_remote_copy(
            src_ref=src,
            dst_ref=dst,
            send_sem=self.send_sems.at[k],
            recv_sem=self.recv_sems.at[k],
            device_id={axis: peer},
            device_id_type=MESH,
        )

    def start(self, copy):
        copy.start()
        self.sent.append(copy)


def layer_kernel(slices, chunks, rows, hop, *refs):
    inputs = 11 if hop else 7
    tok_f, tok_b, w_gate, w_up, w_down, pre_gate, pre_up = refs[:7]
    routes = refs[7:inputs]
    outs = 4 if hop else 3
    out_f, out_b, out_dots = refs[inputs : inputs + 3]
    (
        tok, wc, wd, gat, par, xb, yb, pre, rs1, rs2, rsz, hold, hold2, sums, landed, table,
        table_got, dot_out, dot_in, local_sems, send_sems, recv_sems,
    ) = refs[inputs + outs :]
    device = lax.axis_index("expert")
    me = device % slices
    base = device - me
    lo = me % QUAD
    z = me // QUAD
    depth = slices // QUAD
    xp = base + xor(me, 1)
    yp = base + xor(me, 2)
    zp = [base + xor(z, q) * QUAD + lo for q in range(depth)]
    features, ff = wc.shape[0], wd.shape[0]
    width = features // chunks
    pad = padded(rows)

    def bid(q, mask):
        return xor(z, q) * QUAD + xor(lo, mask)

    def cols_of(j):
        return pl.ds(j * width, width)

    loads = []

    def load(src, dst):
        copy = pltpu.make_async_copy(src, dst, local_sems.at[len(loads)])
        loads.append(copy)
        copy.start()
        return copy

    load_f = [load(tok_f.at[:, cols_of(j)], tok.at[0, :, cols_of(j)]) for j in range(chunks)]

    barrier = pltpu.get_barrier_semaphore()
    peers = [(q, m) for q in range(depth) for m in range(QUAD) if q or m]
    for q, m in peers:
        pl.semaphore_signal(
            barrier, inc=1, device_id={"expert": base + bid(q, m)}, device_id_type=MESH
        )
    greeted = len(peers)
    if hop:
        section = lax.axis_index("section")
        sections = lax.axis_size("section")
        ahead = (section + 1) % sections
        behind = (section + sections - 1) % sections
        for peer in (ahead, behind):
            pl.semaphore_signal(barrier, inc=1, device_id={"section": peer}, device_id_type=MESH)
        greeted += 2

    load_b = [load(tok_b.at[:, cols_of(j)], tok.at[1, :, cols_of(j)]) for j in range(chunks)]
    load_w = []
    for j in range(chunks):
        load_w.append(load(w_gate.at[cols_of(j), :], wc.at[cols_of(j), pl.ds(0, ff)]))
        load_w.append(load(w_up.at[cols_of(j), :], wc.at[cols_of(j), pl.ds(ff, ff)]))
        load_w.append(load(w_down.at[:, cols_of(j)], wd.at[:, cols_of(j)]))

    unpack = selection(chunks, rows, pad)
    pack = selection(chunks, rows, pad, flip=True)

    def choose(mb):
        if not hop:
            shape = (pad, tok.shape[1])
            same = lax.broadcasted_iota(jnp.int32, shape, 0)
            return narrow(
                jnp.where(same == lax.broadcasted_iota(jnp.int32, shape, 1), 1.0, 0.0)
            )
        ids = routes[2 * mb][...]
        slots = slot_table(ids, rows)
        gates = jnp.where(ids == 0, routes[2 * mb + 1][...], 0.0)
        table[mb] = slots * jnp.sum(gates, axis=1, keepdims=True)
        return narrow(jnp.transpose(slots)[:pad])

    def place(mb, chosen, waits):
        for j in range(chunks):
            waits[j].wait()
            picked = dot(chosen, tok[mb, :, cols_of(j)])
            yb[0, pl.ds(j * pad, pad), :] = narrow(picked)
        gat[mb, me] = narrow(dot(pack, yb[0]))

    links = Links(send_sems, recv_sems)

    order = list(range(1, depth)) + [0]
    steps = [(0, q) for q in range(depth)] + [(1, q) for q in order]
    tiles = width // LANES
    cut = tiles // 2 * LANES
    zsend, parts = {}, {}
    own_x, own_y, forward = {}, {}, {}
    r1, r2, rz, dots_sent = {}, {}, {}, {}
    for step in steps:
        mb, q = step
        if step == steps[-1]:
            parts[step] = [(True, pl.ds(0, cut)), (False, pl.ds(cut, width - cut))]
        else:
            parts[step] = [(q % 2 == 0, pl.ds(0, width))]
        if q > 0:
            zsend[step] = links.copy(gat.at[mb, me], gat.at[mb, me], zp[q])
            rz[step] = links.copy(hold2.at[mb, q], rsz.at[mb, q], zp[q])
        own_x[step], own_y[step], forward[step], r1[step], r2[step] = [], [], [], [], []
        for first, cols in parts[step]:
            block = gat.at[mb, bid(q, 0), :, cols]
            own_x[step].append(links.copy(block, block, xp))
            own_y[step].append(links.copy(block, block, yp))
            got = gat.at[mb, bid(q, 2 if first else 1), :, cols]
            forward[step].append(links.copy(got, got, xp if first else yp))
            m1, p1, p2 = (1, xp, yp) if first else (2, yp, xp)
            r1[step].append([
                links.copy(par.at[mb, bid(q, 3), :, cols], rs1.at[mb, q, 1, :, cols], p1),
                links.copy(par.at[mb, bid(q, m1), :, cols], rs1.at[mb, q, 0, :, cols], p1),
            ])
            r2[step].append(links.copy(hold.at[mb, q, :, cols], rs2.at[mb, q, :, cols], p2))
        if mb == 1:
            dots_sent[q] = [
                links.copy(dot_out.at[bid(q, m)], dot_in.at[q * QUAD + m], base + bid(q, m))
                for m in range(QUAD)
                if q or m
            ]
    if hop:
        across = [
            links.copy(sums.at[0], landed.at[0], ahead, "section"),
            links.copy(sums.at[1], landed.at[1], behind, "section"),
        ]
        tables = [
            links.copy(table.at[0], table_got.at[0], ahead, "section"),
            links.copy(table.at[1], table_got.at[1], behind, "section"),
        ]

    def do_own(step):
        if step[1] > 0:
            zsend[step].wait_recv()
        for copy_x, copy_y in zip(own_x[step], own_y[step]):
            links.start(copy_x)
            links.start(copy_y)

    def start_mb(mb):
        for q in range(1, depth):
            links.start(zsend[mb, q])

    def do_forward(step):
        for k, (first, cols) in enumerate(parts[step]):
            (own_y if first else own_x)[step][k].wait_recv()
            links.start(forward[step][k])

    def compute(step):
        mb, q = step
        for k, (first, cols) in enumerate(parts[step]):
            (own_x if first else own_y)[step][k].wait_recv()
            forward[step][k].wait_recv()
        zq = xor(z, q)
        group = zq * QUAD
        for b in range(QUAD):
            full = narrow(dot(unpack, gat[mb, group + b]))
            for j in range(chunks):
                xb[pl.ds(b * pad, pad), cols_of(j)] = full[j * pad : (j + 1) * pad]
        total = None
        for j in range(chunks):
            if mb == 0:
                part = dot(xb[:, cols_of(j)], wc[cols_of(j), :])
            else:
                part = dot(xb[:, cols_of(j)], wd[:, cols_of(j)], ((1,), (1,)))
            total = part if total is None else total + part
        if mb == 0:
            gate = total[:, :ff]
            hidden = narrow(gate / (1.0 + jnp.exp(-gate)) * total[:, ff:])

            def piece(j):
                return dot(hidden, wd[:, cols_of(j)])

        else:
            gate = wide(pre[0, zq])
            up = wide(pre[1, zq])
            sig = 1.0 / (1.0 + jnp.exp(-gate))
            activated = gate * sig
            dots = jnp.sum(total * activated * up, axis=1, keepdims=True)
            shape = (QUAD * pad, LANES)
            inner = lax.broadcasted_iota(jnp.int32, shape, 0) & (pad - 1)
            lane = lax.broadcasted_iota(jnp.int32, shape, 1)
            placed = jnp.where(inner == lane, dots, 0.0)
            for b in range(QUAD):
                line = jnp.sum(placed[b * pad : (b + 1) * pad], axis=0, keepdims=True)
                dot_out[group + b] = jnp.broadcast_to(line, (8, LANES))
            for copy in dots_sent[q]:
                links.start(copy)
            grad_gate = narrow(total * up * sig * (1.0 + gate * (1.0 - sig)))
            both = jnp.concatenate([grad_gate, narrow(total * activated)], axis=1)

            def piece(j):
                return dot(both, wc[cols_of(j), :], ((1,), (1,)))

        for j in range(chunks):
            full = narrow(piece(j))
            for b in range(QUAD):
                yb[b, pl.ds(j * pad, pad), :] = full[b * pad : (b + 1) * pad]
        for b in range(QUAD):
            par[mb, group + b] = narrow(dot(pack, yb[b]))
        for copies in r1[step]:
            for copy in copies:
                links.start(copy)

    def second(step):
        mb, q = step
        for k, (first, cols) in enumerate(parts[step]):
            r1[step][k][0].wait_recv()
            m2 = 2 if first else 1
            total = wide(par[mb, bid(q, m2), :, cols]) + wide(rs1[mb, q, 1, :, cols])
            hold[mb, q, :, cols] = narrow(total)
            links.start(r2[step][k])

    def third(step):
        mb, q = step
        for k, (first, cols) in enumerate(parts[step]):
            r1[step][k][1].wait_recv()
            r2[step][k].wait_recv()
            total = wide(par[mb, bid(q, 0), :, cols]) + wide(rs1[mb, q, 0, :, cols])
            total = total + wide(rs2[mb, q, :, cols])
            hold2[mb, q, :, cols] = narrow(total)
        if q > 0:
            links.start(rz[step])

    def finish(mb):
        total = wide(hold2[mb, 0])
        for q in range(1, depth):
            rz[mb, q].wait_recv()
            total = total + wide(rsz[mb, q])
        sums[mb] = narrow(total)
        if hop:
            links.start(across[mb])

    def deliver(mb, out):
        if hop:
            across[mb].wait_recv()
            out[...] = landed[mb]
        else:
            out[...] = sums[mb]

    place(0, choose(0), load_f)
    pl.semaphore_wait(barrier, greeted)
    do_own(steps[0])
    start_mb(0)
    place(1, choose(1), load_b)
    start_mb(1)
    if hop:
        for copy in tables:
            links.start(copy)
    spaced = selection(slices, rows, pad)
    for k, saved in enumerate((pre_gate, pre_up)):
        pre[k] = narrow(dot(spaced, saved[...])).reshape(pre.shape[1:])

    count = len(steps)
    gathers = [(do_own, s) for s in range(1)]
    for s in range(1, count):
        gathers += [(do_own, s), (do_forward, s - 1)]
    gathers = gathers[1:] + [(do_forward, count - 1)]

    def gather_to(s):
        while gathers and (do_forward, min(s, count - 1)) in gathers:
            event, at = gathers.pop(0)
            event(steps[at])

    for t in range(count + THIRD_LAG):
        gather_to(t + AHEAD - 1)
        if t == 0:
            for copy in load_w:
                copy.wait()
        if t < count:
            compute(steps[t])
        if 0 <= t - SECOND_LAG < count:
            second(steps[t - SECOND_LAG])
        if 0 <= t - THIRD_LAG < count:
            third(steps[t - THIRD_LAG])
        if t == count - 1:
            finish(0)
        if t == count:
            deliver(0, out_f)
    total = dot_out[me]
    for q in range(depth):
        for copy in dots_sent[q]:
            copy.wait_recv()
    for q, m in peers:
        total = total + dot_in[q * QUAD + m]
    out_dots[...] = total
    if hop:
        out_tables = refs[inputs + 3]
        for k in range(2):
            tables[k].wait_recv()
            out_tables[k] = table_got[k]
    finish(1)
    deliver(1, out_b)
    for copy in links.sent:
        copy.wait_send()


def run_layer(tok_f, tok_b, w_gate, w_up, w_down, pre_gate, pre_up, routes, slices, rows):
    hop = bool(routes)
    features = tok_f.shape[1]
    chunks = 16 // math.gcd(16, rows)
    width = features // chunks
    ff = w_gate.shape[1]
    depth = slices // QUAD
    pad = padded(rows)
    group = QUAD * pad

    vmem = pl.BlockSpec(memory_space=pltpu.VMEM)
    anywhere = pl.BlockSpec(memory_space=pl.ANY)
    block = (chunks * rows, width)
    tables = (2, tok_f.shape[0] if hop else 8, LANES)
    out_shape = [
        jax.ShapeDtypeStruct(block, jnp.bfloat16),
        jax.ShapeDtypeStruct(block, jnp.bfloat16),
        jax.ShapeDtypeStruct((8, LANES), jnp.float32),
    ]
    if hop:
        out_shape.append(jax.ShapeDtypeStruct(tables, jnp.float32))
    return pl.pallas_call(
        functools.partial(layer_kernel, slices, chunks, rows, hop),
        out_shape=tuple(out_shape),
        in_specs=[anywhere] * 5 + [vmem] * (2 + len(routes)),
        out_specs=(vmem,) * len(out_shape),
        scratch_shapes=[
            pltpu.VMEM((2,) + tok_f.shape, jnp.bfloat16),
            pltpu.VMEM((features, 2 * ff), jnp.bfloat16),
            pltpu.VMEM((ff, features), jnp.bfloat16),
            pltpu.VMEM((2, slices) + block, jnp.bfloat16),
            pltpu.VMEM((2, slices) + block, jnp.bfloat16),
            pltpu.VMEM((group, features), jnp.bfloat16),
            pltpu.VMEM((QUAD, chunks * pad, width), jnp.bfloat16),
            pltpu.VMEM((2, depth, group, ff), jnp.bfloat16),
            pltpu.VMEM((2, depth, 2) + block, jnp.bfloat16),
            pltpu.VMEM((2, depth) + block, jnp.bfloat16),
            pltpu.VMEM((2, depth) + block, jnp.bfloat16),
            pltpu.VMEM((2, depth) + block, jnp.bfloat16),
            pltpu.VMEM((2, depth) + block, jnp.bfloat16),
            pltpu.VMEM((2,) + block, jnp.bfloat16),
            pltpu.VMEM((2,) + block, jnp.bfloat16),
            pltpu.VMEM(tables, jnp.float32),
            pltpu.VMEM(tables, jnp.float32),
            pltpu.VMEM((slices, 8, LANES), jnp.float32),
            pltpu.VMEM((slices, 8, LANES), jnp.float32),
            pltpu.SemaphoreType.DMA((5 * chunks,)),
            pltpu.SemaphoreType.DMA((SEMAPHORES,)),
            pltpu.SemaphoreType.DMA((SEMAPHORES,)),
        ],
        compiler_params=pltpu.CompilerParams(
            collective_id=0, has_side_effects=True, vmem_limit_bytes=56 * 2**20
        ),
        name="moe_layer",
    )(tok_f, tok_b, w_gate, w_up, w_down, pre_gate, pre_up, *routes)


def mix_kernel(rows, graded, *refs):
    block_f, block_b, tables = refs[:3]
    extra = 2 if graded else 0
    outs = refs[3 + extra : 5 + extra]
    stage, sems = refs[-2:]
    block_rows, width = block_f.shape
    chunks = block_rows // rows
    pad = padded(rows)
    unpack = selection(chunks, rows, pad)
    copies = []
    for k, block in enumerate((block_f, block_b)):
        weight = tables[k][:, :pad]
        high = narrow(weight)
        both = jnp.concatenate([high, narrow(weight - wide(high))], axis=1)
        full = narrow(dot(unpack, block[...]))
        for j in range(chunks):
            part = full[j * pad : (j + 1) * pad]
            cols = pl.ds(j * width, width)
            stage[k, :, cols] = narrow(dot(both, jnp.concatenate([part, part], axis=0)))
            copies.append(
                pltpu.make_async_copy(
                    stage.at[k, :, cols], outs[k].at[:, cols], sems.at[k * chunks + j]
                )
            )
            copies[-1].start()
    if graded:
        dots, ids = refs[3], refs[4]
        slots = slot_table(ids[...], rows)
        found = jnp.sum(slots * dots[:1], axis=1, keepdims=True)
        refs[7][...] = jnp.where(ids[...] == 0, found, 0.0)
    for copy in copies:
        copy.wait()


def mix(block_f, block_b, tables, rows, grading):
    block_rows, width = block_f.shape
    tokens = tables.shape[1]
    chunks = block_rows // rows
    vmem = pl.BlockSpec(memory_space=pltpu.VMEM)
    anywhere = pl.BlockSpec(memory_space=pl.ANY)
    shape = jax.ShapeDtypeStruct((tokens, chunks * width), jnp.bfloat16)
    out_shape = [shape, shape]
    if grading:
        out_shape.append(jax.ShapeDtypeStruct(grading[1].shape, jnp.float32))
    return pl.pallas_call(
        functools.partial(mix_kernel, rows, bool(grading)),
        out_shape=tuple(out_shape),
        in_specs=[vmem] * (3 + len(grading)),
        out_specs=tuple([anywhere, anywhere] + [vmem] * (len(out_shape) - 2)),
        scratch_shapes=[
            pltpu.VMEM((2, tokens, chunks * width), jnp.bfloat16),
            pltpu.SemaphoreType.DMA((2 * chunks,)),
        ],
        name="mix",
    )(block_f, block_b, tables, *grading)


def body(
    act_in,
    cotangent,
    fwd_ids,
    fwd_gates,
    bwd_ids,
    bwd_gates,
    gate_w,
    up_w,
    down_w,
    gate_pre,
    up_pre,
):
    ndev = lax.axis_size("expert")
    ff_dev = gate_w.shape[2]
    slices = FF // ff_dev
    experts = ndev // slices
    capacity = gate_pre.shape[1] // ndev
    rows = experts * capacity
    weights = (gate_w[0], up_w[0], down_w[0])

    if experts == 1:
        routes = (fwd_ids[0], fwd_gates[0], bwd_ids[0], bwd_gates[0])
        block_f, block_b, dots, tables = run_layer(
            act_in[0], cotangent[0], *weights, gate_pre[0], up_pre[0], routes, slices, rows
        )
        outs = mix(block_f, block_b, tables, rows, (dots, bwd_ids[0]))
        return tuple(out[None] for out in outs)

    chunks = 16 // math.gcd(16, rows)
    features = act_in.shape[2]
    width = features // chunks
    columns = [[g * slices + i for g in range(experts)] for i in range(slices)]

    def exchange(value):
        return lax.all_to_all(
            value, "expert", split_axis=0, concat_axis=0, axis_index_groups=columns, tiled=True
        )

    matches_f, placing_f, weights_f = routing(fwd_ids[0], fwd_gates[0], experts, capacity)
    matches_b, placing_b, weights_b = routing(bwd_ids[0], bwd_gates[0], experts, capacity)

    def prepare(tokens, placing):
        chosen = placing.reshape(rows, tokens.shape[0])
        picked = dot(chosen.astype(jnp.bfloat16), tokens).astype(jnp.bfloat16)
        picked = exchange(picked.reshape(experts, capacity, features))
        return picked.reshape(rows, features)

    def by_group(saved):
        saved = saved.reshape(experts, slices, capacity, ff_dev).transpose(1, 0, 2, 3)
        return saved.reshape(slices * rows, ff_dev)

    block_f, block_b, dots = run_layer(
        prepare(act_in[0], placing_f), prepare(cotangent[0], placing_b), *weights,
        by_group(gate_pre[0]), by_group(up_pre[0]), (), slices, rows,
    )
    mine = exchange(dots[0, :rows].reshape(experts, capacity))

    def send_back(block):
        table = block.reshape(chunks, rows, width).transpose(1, 0, 2)
        table = exchange(table.reshape(experts, capacity, features))
        table = table.reshape(rows, chunks, width).transpose(1, 0, 2)
        return table.reshape(chunks * rows, width)

    token_dots = jnp.sum(placing_b * mine[:, :, None], axis=1)
    gate_grad = jnp.sum(jnp.where(matches_b, token_dots[:, :, None], 0.0), axis=0)

    def weight_table(placing, weights):
        table = (placing * weights[:, None, :]).reshape(rows, -1).T
        return jnp.pad(table, ((0, 0), (0, LANES - rows)))

    def onward(block, placing, weights, step):
        block = from_behind(send_back(block), "section", step)
        return block, from_behind(weight_table(placing, weights), "section", step)

    block_f, table_f = onward(block_f, placing_f, weights_f, 1)
    block_b, table_b = onward(block_b, placing_b, weights_b, -1)
    next_act, prev_grad = mix(block_f, block_b, jnp.stack([table_f, table_b]), rows, ())
    return (next_act[None], prev_grad[None], gate_grad[None])


def solution(mesh):
    in_specs = (
        P("section", "expert", None),
        P("section", "expert", None),
        P("section", "expert", None),
        P("section", "expert", None),
        P("section", "expert", None),
        P("section", "expert", None),
        P("section", None, "expert"),
        P("section", None, "expert"),
        P("section", "expert", None),
        P("section", None, "expert"),
        P("section", None, "expert"),
    )
    out_specs = (
        P("section", "expert", None),
        P("section", "expert", None),
        P("section", "expert", None),
    )
    return jax.shard_map(body, mesh=mesh, in_specs=in_specs, out_specs=out_specs, check_vma=False)
```

```python
import functools
import math

import jax
import jax.numpy as jnp
from jax import lax
from jax.experimental import pallas as pl
from jax.experimental.pallas import tpu as pltpu
from jax.sharding import PartitionSpec as P

FF = 2048
QUAD = 4
LANES = 128
AHEAD = 3
SECOND_LAG = 1
THIRD_LAG = 2
SEMAPHORES = 128
MESH = pl.DeviceIdType.MESH


def from_behind(value, axis, steps):
    count = lax.axis_size(axis)
    pairs = [(source, (source + steps) % count) for source in range(count)]
    return lax.ppermute(value, axis, pairs)


def routing(ids, gates, experts, capacity):
    expert_ids = jnp.arange(experts, dtype=jnp.int32)
    matches = ids[None, :, :] == expert_ids[:, None, None]
    routed = jnp.any(matches, axis=2)
    weights = jnp.sum(jnp.where(matches, gates[None, :, :], 0.0), axis=2)
    tokens = ids.shape[0]
    earlier = jnp.arange(tokens)[:, None] <= jnp.arange(tokens)[None, :]
    counted = jnp.sum(jnp.where(routed[:, :, None] & earlier[None], 1, 0), axis=1)
    position = counted - 1
    slot_ids = jnp.arange(capacity, dtype=jnp.int32)
    placing = (position[:, None, :] == slot_ids[None, :, None]) & routed[:, None, :]
    return (matches, placing.astype(jnp.float32), weights)


def xor(value, mask):
    out = value
    bit = 1
    while bit <= mask:
        if mask & bit:
            out = out + bit - 2 * bit * ((value // bit) % 2)
        bit *= 2
    return out


def dot(a, b, dims=((1,), (0,))):
    return lax.dot_general(a, b, (dims, ((), ())), preferred_element_type=jnp.float32)


def wide(value):
    return value.astype(jnp.float32)


def narrow(value):
    return value.astype(jnp.bfloat16)


def padded(rows):
    return -(-rows // 16) * 16


def selection(count, rows, pad, flip=False):
    shape = (count * rows, count * pad) if flip else (count * pad, count * rows)
    long = lax.broadcasted_iota(jnp.int32, shape, 1 if flip else 0)
    short = lax.broadcasted_iota(jnp.int32, shape, 0 if flip else 1)
    piece = lax.shift_right_logical(long, jnp.int32(pad.bit_length() - 1))
    inner = long & (pad - 1)
    chosen = (short == piece * rows + inner) & (inner < rows)
    return narrow(jnp.where(chosen, 1.0, 0.0))


def slot_rows(ids, count):
    tokens = ids.shape[1]
    routed = jnp.max(jnp.where(ids == 0, 1.0, 0.0), axis=0, keepdims=True)
    spread = jnp.broadcast_to(routed, (count, tokens))
    row = lax.broadcasted_iota(jnp.int32, (tokens, tokens), 0)
    column = lax.broadcasted_iota(jnp.int32, (tokens, tokens), 1)
    upper = narrow(jnp.where(row <= column, 1.0, 0.0))
    rank = dot(narrow(spread), upper) - 1.0
    slot = wide(lax.broadcasted_iota(jnp.int32, (count, tokens), 0))
    return jnp.where((rank == slot) & (spread > 0.0), 1.0, 0.0)


class Links:
    def __init__(self, send_sems, recv_sems):
        self.send_sems = send_sems
        self.recv_sems = recv_sems
        self.count = 0
        self.sent = []

    def copy(self, src, dst, peer, axis="expert"):
        k = self.count
        self.count += 1
        assert k < SEMAPHORES
        return pltpu.make_async_remote_copy(
            src_ref=src,
            dst_ref=dst,
            send_sem=self.send_sems.at[k],
            recv_sem=self.recv_sems.at[k],
            device_id={axis: peer},
            device_id_type=MESH,
        )

    def start(self, copy):
        copy.start()
        self.sent.append(copy)


def layer_kernel(slices, chunks, rows, hop, *refs):
    inputs = 11 if hop else 7
    tok_f, tok_b, w_gate, w_up, w_down, pre_gate, pre_up = refs[:7]
    routes = refs[7:inputs]
    outs = 4 if hop else 3
    out_f, out_b, out_dots = refs[inputs : inputs + 3]
    (
        tok, wc, wd, gat, par, xb, yb, pre, rs1, rs2, rsz, hold, hold2, sums, landed, table,
        table_got, dot_out, dot_in, local_sems, send_sems, recv_sems,
    ) = refs[inputs + outs :]
    device = lax.axis_index("expert")
    me = device % slices
    base = device - me
    lo = me % QUAD
    z = me // QUAD
    depth = slices // QUAD
    xp = base + xor(me, 1)
    yp = base + xor(me, 2)
    zp = [base + xor(z, q) * QUAD + lo for q in range(depth)]
    features, ff = wc.shape[0], wd.shape[0]
    width = features // chunks
    pad = padded(rows)

    def bid(q, mask):
        return xor(z, q) * QUAD + xor(lo, mask)

    def cols_of(j):
        return pl.ds(j * width, width)

    loads = []

    def load(src, dst):
        copy = pltpu.make_async_copy(src, dst, local_sems.at[len(loads)])
        loads.append(copy)
        copy.start()
        return copy

    load_f = [load(tok_f.at[:, cols_of(j)], tok.at[0, :, cols_of(j)]) for j in range(chunks)]

    barrier = pltpu.get_barrier_semaphore()
    peers = [(q, m) for q in range(depth) for m in range(QUAD) if q or m]
    for q, m in peers:
        pl.semaphore_signal(
            barrier, inc=1, device_id={"expert": base + bid(q, m)}, device_id_type=MESH
        )
    greeted = len(peers)
    if hop:
        section = lax.axis_index("section")
        sections = lax.axis_size("section")
        ahead = (section + 1) % sections
        behind = (section + sections - 1) % sections
        for peer in (ahead, behind):
            pl.semaphore_signal(barrier, inc=1, device_id={"section": peer}, device_id_type=MESH)
        greeted += 2

    load_b = [load(tok_b.at[:, cols_of(j)], tok.at[1, :, cols_of(j)]) for j in range(chunks)]
    load_w = []
    for j in range(chunks):
        load_w.append(load(w_gate.at[cols_of(j), :], wc.at[cols_of(j), pl.ds(0, ff)]))
        load_w.append(load(w_up.at[cols_of(j), :], wc.at[cols_of(j), pl.ds(ff, ff)]))
        load_w.append(load(w_down.at[:, cols_of(j)], wd.at[:, cols_of(j)]))

    unpack = selection(chunks, rows, pad)
    pack = selection(chunks, rows, pad, flip=True)

    def choose(mb):
        if not hop:
            shape = (pad, tok.shape[1])
            same = lax.broadcasted_iota(jnp.int32, shape, 0)
            return narrow(
                jnp.where(same == lax.broadcasted_iota(jnp.int32, shape, 1), 1.0, 0.0)
            )
        ids = routes[2 * mb][...]
        slots = slot_rows(ids, LANES)
        gates = jnp.where(ids == 0, routes[2 * mb + 1][...], 0.0)
        table[mb] = jnp.transpose(slots * jnp.sum(gates, axis=0, keepdims=True))
        return narrow(slots[:pad])

    def place(mb, chosen, waits):
        for j in range(chunks):
            waits[j].wait()
            picked = dot(chosen, tok[mb, :, cols_of(j)])
            yb[0, pl.ds(j * pad, pad), :] = narrow(picked)
        gat[mb, me] = narrow(dot(pack, yb[0]))

    links = Links(send_sems, recv_sems)

    order = list(range(1, depth)) + [0]
    steps = [(0, q) for q in range(depth)] + [(1, q) for q in order]
    tiles = width // LANES
    cut = tiles // 2 * LANES
    zsend, parts = {}, {}
    own_x, own_y, forward = {}, {}, {}
    r1, r2, rz, dots_sent = {}, {}, {}, {}
    for step in steps:
        mb, q = step
        if step == steps[-1]:
            parts[step] = [(True, pl.ds(0, cut)), (False, pl.ds(cut, width - cut))]
        else:
            parts[step] = [(q % 2 == 0, pl.ds(0, width))]
        if q > 0:
            zsend[step] = links.copy(gat.at[mb, me], gat.at[mb, me], zp[q])
            rz[step] = links.copy(hold2.at[mb, q], rsz.at[mb, q], zp[q])
        own_x[step], own_y[step], forward[step], r1[step], r2[step] = [], [], [], [], []
        for first, cols in parts[step]:
            block = gat.at[mb, bid(q, 0), :, cols]
            own_x[step].append(links.copy(block, block, xp))
            own_y[step].append(links.copy(block, block, yp))
            got = gat.at[mb, bid(q, 2 if first else 1), :, cols]
            forward[step].append(links.copy(got, got, xp if first else yp))
            m1, p1, p2 = (1, xp, yp) if first else (2, yp, xp)
            r1[step].append([
                links.copy(par.at[mb, bid(q, 3), :, cols], rs1.at[mb, q, 1, :, cols], p1),
                links.copy(par.at[mb, bid(q, m1), :, cols], rs1.at[mb, q, 0, :, cols], p1),
            ])
            r2[step].append(links.copy(hold.at[mb, q, :, cols], rs2.at[mb, q, :, cols], p2))
        if mb == 1:
            dots_sent[q] = [
                links.copy(dot_out.at[bid(q, m)], dot_in.at[q * QUAD + m], base + bid(q, m))
                for m in range(QUAD)
                if q or m
            ]
    if hop:
        across = [
            links.copy(sums.at[0], landed.at[0], ahead, "section"),
            links.copy(sums.at[1], landed.at[1], behind, "section"),
        ]
        tables = [
            links.copy(table.at[0], table_got.at[0], ahead, "section"),
            links.copy(table.at[1], table_got.at[1], behind, "section"),
        ]

    def do_own(step):
        if step[1] > 0:
            zsend[step].wait_recv()
        for copy_x, copy_y in zip(own_x[step], own_y[step]):
            links.start(copy_x)
            links.start(copy_y)

    def start_mb(mb):
        for q in range(1, depth):
            links.start(zsend[mb, q])

    def do_forward(step):
        for k, (first, cols) in enumerate(parts[step]):
            (own_y if first else own_x)[step][k].wait_recv()
            links.start(forward[step][k])

    def compute(step):
        mb, q = step
        for k, (first, cols) in enumerate(parts[step]):
            (own_x if first else own_y)[step][k].wait_recv()
            forward[step][k].wait_recv()
        zq = xor(z, q)
        group = zq * QUAD
        for b in range(QUAD):
            full = narrow(dot(unpack, gat[mb, group + b]))
            for j in range(chunks):
                xb[pl.ds(b * pad, pad), cols_of(j)] = full[j * pad : (j + 1) * pad]
        total = None
        for j in range(chunks):
            if mb == 0:
                part = dot(xb[:, cols_of(j)], wc[cols_of(j), :])
            else:
                part = dot(xb[:, cols_of(j)], wd[:, cols_of(j)], ((1,), (1,)))
            total = part if total is None else total + part
        if mb == 0:
            gate = total[:, :ff]
            hidden = narrow(gate / (1.0 + jnp.exp(-gate)) * total[:, ff:])

            def piece(j):
                return dot(hidden, wd[:, cols_of(j)])

        else:
            gate = wide(pre[0, zq])
            up = wide(pre[1, zq])
            sig = 1.0 / (1.0 + jnp.exp(-gate))
            activated = gate * sig
            dots = jnp.sum(total * activated * up, axis=1, keepdims=True)
            for b in range(QUAD):
                mine = dots[b * pad : (b + 1) * pad]
                dot_out[group + b] = jnp.broadcast_to(mine, (pad, LANES))
            for copy in dots_sent[q]:
                links.start(copy)
            grad_gate = narrow(total * up * sig * (1.0 + gate * (1.0 - sig)))
            both = jnp.concatenate([grad_gate, narrow(total * activated)], axis=1)

            def piece(j):
                return dot(both, wc[cols_of(j), :], ((1,), (1,)))

        for j in range(chunks):
            full = narrow(piece(j))
            for b in range(QUAD):
                yb[b, pl.ds(j * pad, pad), :] = full[b * pad : (b + 1) * pad]
        for b in range(QUAD):
            par[mb, group + b] = narrow(dot(pack, yb[b]))
        for copies in r1[step]:
            for copy in copies:
                links.start(copy)

    def second(step):
        mb, q = step
        for k, (first, cols) in enumerate(parts[step]):
            r1[step][k][0].wait_recv()
            m2 = 2 if first else 1
            total = wide(par[mb, bid(q, m2), :, cols]) + wide(rs1[mb, q, 1, :, cols])
            hold[mb, q, :, cols] = narrow(total)
            links.start(r2[step][k])

    def third(step):
        mb, q = step
        for k, (first, cols) in enumerate(parts[step]):
            r1[step][k][1].wait_recv()
            r2[step][k].wait_recv()
            total = wide(par[mb, bid(q, 0), :, cols]) + wide(rs1[mb, q, 0, :, cols])
            total = total + wide(rs2[mb, q, :, cols])
            hold2[mb, q, :, cols] = narrow(total)
        if q > 0:
            links.start(rz[step])

    def finish(mb):
        total = wide(hold2[mb, 0])
        for q in range(1, depth):
            rz[mb, q].wait_recv()
            total = total + wide(rsz[mb, q])
        sums[mb] = narrow(total)
        if hop:
            links.start(across[mb])

    def deliver(mb, out):
        if hop:
            across[mb].wait_recv()
            out[...] = landed[mb]
        else:
            out[...] = sums[mb]

    place(0, choose(0), load_f)
    pl.semaphore_wait(barrier, greeted)
    do_own(steps[0])
    start_mb(0)
    place(1, choose(1), load_b)
    start_mb(1)
    if hop:
        for copy in tables:
            links.start(copy)
    spaced = selection(slices, rows, pad)
    for k, saved in enumerate((pre_gate, pre_up)):
        pre[k] = narrow(dot(spaced, saved[...])).reshape(pre.shape[1:])

    count = len(steps)
    gathers = [(do_own, s) for s in range(1)]
    for s in range(1, count):
        gathers += [(do_own, s), (do_forward, s - 1)]
    gathers = gathers[1:] + [(do_forward, count - 1)]

    def gather_to(s):
        while gathers and (do_forward, min(s, count - 1)) in gathers:
            event, at = gathers.pop(0)
            event(steps[at])

    for t in range(count + THIRD_LAG):
        gather_to(t + AHEAD - 1)
        if t == 0:
            for copy in load_w:
                copy.wait()
        if t < count:
            compute(steps[t])
        if 0 <= t - SECOND_LAG < count:
            second(steps[t - SECOND_LAG])
        if 0 <= t - THIRD_LAG < count:
            third(steps[t - THIRD_LAG])
        if t == count - 1:
            finish(0)
        if t == count:
            deliver(0, out_f)
    total = dot_out[me]
    for q in range(depth):
        for copy in dots_sent[q]:
            copy.wait_recv()
    for q, m in peers:
        total = total + dot_in[q * QUAD + m]
    out_dots[...] = total
    if hop:
        out_tables = refs[inputs + 3]
        for k in range(2):
            tables[k].wait_recv()
            out_tables[k] = table_got[k]
    finish(1)
    deliver(1, out_b)
    for copy in links.sent:
        copy.wait_send()


def run_layer(tok_f, tok_b, w_gate, w_up, w_down, pre_gate, pre_up, routes, slices, rows):
    hop = bool(routes)
    features = tok_f.shape[1]
    chunks = 16 // math.gcd(16, rows)
    width = features // chunks
    ff = w_gate.shape[1]
    depth = slices // QUAD
    pad = padded(rows)
    group = QUAD * pad

    vmem = pl.BlockSpec(memory_space=pltpu.VMEM)
    anywhere = pl.BlockSpec(memory_space=pl.ANY)
    block = (chunks * rows, width)
    tables = (2, tok_f.shape[0] if hop else 8, LANES)
    out_shape = [
        jax.ShapeDtypeStruct(block, jnp.bfloat16),
        jax.ShapeDtypeStruct(block, jnp.bfloat16),
        jax.ShapeDtypeStruct((pad, LANES), jnp.float32),
    ]
    if hop:
        out_shape.append(jax.ShapeDtypeStruct(tables, jnp.float32))
    return pl.pallas_call(
        functools.partial(layer_kernel, slices, chunks, rows, hop),
        out_shape=tuple(out_shape),
        in_specs=[anywhere] * 5 + [vmem] * (2 + len(routes)),
        out_specs=(vmem,) * len(out_shape),
        scratch_shapes=[
            pltpu.VMEM((2,) + tok_f.shape, jnp.bfloat16),
            pltpu.VMEM((features, 2 * ff), jnp.bfloat16),
            pltpu.VMEM((ff, features), jnp.bfloat16),
            pltpu.VMEM((2, slices) + block, jnp.bfloat16),
            pltpu.VMEM((2, slices) + block, jnp.bfloat16),
            pltpu.VMEM((group, features), jnp.bfloat16),
            pltpu.VMEM((QUAD, chunks * pad, width), jnp.bfloat16),
            pltpu.VMEM((2, depth, group, ff), jnp.bfloat16),
            pltpu.VMEM((2, depth, 2) + block, jnp.bfloat16),
            pltpu.VMEM((2, depth) + block, jnp.bfloat16),
            pltpu.VMEM((2, depth) + block, jnp.bfloat16),
            pltpu.VMEM((2, depth) + block, jnp.bfloat16),
            pltpu.VMEM((2, depth) + block, jnp.bfloat16),
            pltpu.VMEM((2,) + block, jnp.bfloat16),
            pltpu.VMEM((2,) + block, jnp.bfloat16),
            pltpu.VMEM(tables, jnp.float32),
            pltpu.VMEM(tables, jnp.float32),
            pltpu.VMEM((slices, pad, LANES), jnp.float32),
            pltpu.VMEM((slices, pad, LANES), jnp.float32),
            pltpu.SemaphoreType.DMA((5 * chunks,)),
            pltpu.SemaphoreType.DMA((SEMAPHORES,)),
            pltpu.SemaphoreType.DMA((SEMAPHORES,)),
        ],
        compiler_params=pltpu.CompilerParams(
            collective_id=0, has_side_effects=True, vmem_limit_bytes=56 * 2**20
        ),
        name="moe_layer",
    )(tok_f, tok_b, w_gate, w_up, w_down, pre_gate, pre_up, *routes)


def mix_kernel(rows, graded, *refs):
    block_f, block_b, tables = refs[:3]
    extra = 2 if graded else 0
    outs = refs[3 + extra : 5 + extra]
    stage, sems = refs[-2:]
    block_rows, width = block_f.shape
    chunks = block_rows // rows
    pad = padded(rows)
    unpack = selection(chunks, rows, pad)
    copies = []
    for k, block in enumerate((block_f, block_b)):
        weight = tables[k][:, :pad]
        high = narrow(weight)
        both = jnp.concatenate([high, narrow(weight - wide(high))], axis=1)
        full = narrow(dot(unpack, block[...]))
        for j in range(chunks):
            part = full[j * pad : (j + 1) * pad]
            cols = pl.ds(j * width, width)
            stage[k, :, cols] = narrow(dot(both, jnp.concatenate([part, part], axis=0)))
            copies.append(
                pltpu.make_async_copy(
                    stage.at[k, :, cols], outs[k].at[:, cols], sems.at[k * chunks + j]
                )
            )
            copies[-1].start()
    if graded:
        dots, ids = refs[3], refs[4]
        slots = slot_rows(ids[...], pad)
        found = jnp.sum(slots * dots[...], axis=0, keepdims=True)
        refs[7][...] = jnp.where(ids[...] == 0, found, 0.0)
    for copy in copies:
        copy.wait()


def mix(block_f, block_b, tables, rows, grading):
    block_rows, width = block_f.shape
    tokens = tables.shape[1]
    chunks = block_rows // rows
    vmem = pl.BlockSpec(memory_space=pltpu.VMEM)
    anywhere = pl.BlockSpec(memory_space=pl.ANY)
    shape = jax.ShapeDtypeStruct((tokens, chunks * width), jnp.bfloat16)
    out_shape = [shape, shape]
    if grading:
        out_shape.append(jax.ShapeDtypeStruct(grading[1].shape, jnp.float32))
    return pl.pallas_call(
        functools.partial(mix_kernel, rows, bool(grading)),
        out_shape=tuple(out_shape),
        in_specs=[vmem] * (3 + len(grading)),
        out_specs=tuple([anywhere, anywhere] + [vmem] * (len(out_shape) - 2)),
        scratch_shapes=[
            pltpu.VMEM((2, tokens, chunks * width), jnp.bfloat16),
            pltpu.SemaphoreType.DMA((2 * chunks,)),
        ],
        name="mix",
    )(block_f, block_b, tables, *grading)


def body(
    act_in,
    cotangent,
    fwd_ids,
    fwd_gates,
    bwd_ids,
    bwd_gates,
    gate_w,
    up_w,
    down_w,
    gate_pre,
    up_pre,
):
    ndev = lax.axis_size("expert")
    ff_dev = gate_w.shape[2]
    slices = FF // ff_dev
    experts = ndev // slices
    capacity = gate_pre.shape[1] // ndev
    rows = experts * capacity
    weights = (gate_w[0], up_w[0], down_w[0])

    if experts == 1:
        routes = tuple(each[0].T for each in (fwd_ids, fwd_gates, bwd_ids, bwd_gates))
        block_f, block_b, dots, tables = run_layer(
            act_in[0], cotangent[0], *weights, gate_pre[0], up_pre[0], routes, slices, rows
        )
        next_act, prev_grad, grads = mix(block_f, block_b, tables, rows, (dots, routes[2]))
        return (next_act[None], prev_grad[None], grads.T[None])

    chunks = 16 // math.gcd(16, rows)
    features = act_in.shape[2]
    width = features // chunks
    columns = [[g * slices + i for g in range(experts)] for i in range(slices)]

    def exchange(value):
        return lax.all_to_all(
            value, "expert", split_axis=0, concat_axis=0, axis_index_groups=columns, tiled=True
        )

    matches_f, placing_f, weights_f = routing(fwd_ids[0], fwd_gates[0], experts, capacity)
    matches_b, placing_b, weights_b = routing(bwd_ids[0], bwd_gates[0], experts, capacity)

    def prepare(tokens, placing):
        chosen = placing.reshape(rows, tokens.shape[0])
        picked = dot(chosen.astype(jnp.bfloat16), tokens).astype(jnp.bfloat16)
        picked = exchange(picked.reshape(experts, capacity, features))
        return picked.reshape(rows, features)

    def by_group(saved):
        saved = saved.reshape(experts, slices, capacity, ff_dev).transpose(1, 0, 2, 3)
        return saved.reshape(slices * rows, ff_dev)

    block_f, block_b, dots = run_layer(
        prepare(act_in[0], placing_f), prepare(cotangent[0], placing_b), *weights,
        by_group(gate_pre[0]), by_group(up_pre[0]), (), slices, rows,
    )
    mine = exchange(dots[:rows, 0].reshape(experts, capacity))

    def send_back(block):
        table = block.reshape(chunks, rows, width).transpose(1, 0, 2)
        table = exchange(table.reshape(experts, capacity, features))
        table = table.reshape(rows, chunks, width).transpose(1, 0, 2)
        return table.reshape(chunks * rows, width)

    token_dots = jnp.sum(placing_b * mine[:, :, None], axis=1)
    gate_grad = jnp.sum(jnp.where(matches_b, token_dots[:, :, None], 0.0), axis=0)

    def weight_table(placing, weights):
        table = (placing * weights[:, None, :]).reshape(rows, -1).T
        return jnp.pad(table, ((0, 0), (0, LANES - rows)))

    def onward(block, placing, weights, step):
        block = from_behind(send_back(block), "section", step)
        return block, from_behind(weight_table(placing, weights), "section", step)

    block_f, table_f = onward(block_f, placing_f, weights_f, 1)
    block_b, table_b = onward(block_b, placing_b, weights_b, -1)
    next_act, prev_grad = mix(block_f, block_b, jnp.stack([table_f, table_b]), rows, ())
    return (next_act[None], prev_grad[None], gate_grad[None])


def solution(mesh):
    in_specs = (
        P("section", "expert", None),
        P("section", "expert", None),
        P("section", "expert", None),
        P("section", "expert", None),
        P("section", "expert", None),
        P("section", "expert", None),
        P("section", None, "expert"),
        P("section", None, "expert"),
        P("section", "expert", None),
        P("section", None, "expert"),
        P("section", None, "expert"),
    )
    out_specs = (
        P("section", "expert", None),
        P("section", "expert", None),
        P("section", "expert", None),
    )
    return jax.shard_map(body, mesh=mesh, in_specs=in_specs, out_specs=out_specs, check_vma=False)
```

```python
import functools
import math

import jax
import jax.numpy as jnp
from jax import lax
from jax.experimental import pallas as pl
from jax.experimental.pallas import tpu as pltpu
from jax.sharding import PartitionSpec as P

FF = 2048
QUAD = 4
LANES = 128
SEMAPHORES = 160
TABLES_AFTER = "fwd 0 B"
MESH = pl.DeviceIdType.MESH

SCHEDULE = (
    "place 0", "zs 0 2", "own 0 B", "place 1", "zs 1 1", "own 1 0", "own 1 B", "zs 0 1",
    "zs 0 3", "zs 1 2", "own 0 0", "fwd 1 0", "own 0 2", "own 1 1", "fwd 0 0", "own 0 3",
    "fwd 1 B", "zs 1 3", "fwd 0 B", "fwd 1 1", "own 0 1", "fwd 0 2", "own 1 2", "zB 0 1",
    "zB 0 2", "zB 0 3", "fwd 0 3", "comp 0 0", "zB 1 2", "fwd 1 2", "fwd 0 1", "zB 1 3",
    "own 1 3", "comp 0 2", "comp 0 3", "fwd 1 3", "comp 0 1", "sec 0 2", "comp 1 2", "sec 0 3",
    "zB 1 1", "thi 0 2", "comp 1 3", "sec 0 1", "sec 1 2", "sumB 0", "comp 1 1", "thi 0 3",
    "sec 1 3", "thi 0 1", "sec 1 1", "comp 1 0", "thi 1 2", "sec 0 0", "thi 1 3", "thi 1 1",
    "sec 0 B", "sumB 1", "sec 1 0", "thi 0 B", "sec 1 B", "thi 1 B", "thi 0 0", "thi 1 0",
    "fin 0", "fin 1", "del 0", "del 1",
)
GATHER_X = (
    {"B": True, 0: False, 1: False, 2: True, 3: False},
    {"B": True, 0: True, 1: False, 2: False, 3: False},
)
REDUCE_X = (
    {"B": True, 0: True, 1: True, 2: True, 3: True},
    {"B": False, 0: True, 1: False, 2: False, 3: True},
)


def from_behind(value, axis, steps):
    count = lax.axis_size(axis)
    pairs = [(source, (source + steps) % count) for source in range(count)]
    return lax.ppermute(value, axis, pairs)


def routing(ids, gates, experts, capacity):
    expert_ids = jnp.arange(experts, dtype=jnp.int32)
    matches = ids[None, :, :] == expert_ids[:, None, None]
    routed = jnp.any(matches, axis=2)
    weights = jnp.sum(jnp.where(matches, gates[None, :, :], 0.0), axis=2)
    tokens = ids.shape[0]
    earlier = jnp.arange(tokens)[:, None] <= jnp.arange(tokens)[None, :]
    counted = jnp.sum(jnp.where(routed[:, :, None] & earlier[None], 1, 0), axis=1)
    position = counted - 1
    slot_ids = jnp.arange(capacity, dtype=jnp.int32)
    placing = (position[:, None, :] == slot_ids[None, :, None]) & routed[:, None, :]
    return (matches, placing.astype(jnp.float32), weights)


def xor(value, mask):
    out = value
    bit = 1
    while bit <= mask:
        if mask & bit:
            out = out + bit - 2 * bit * ((value // bit) % 2)
        bit *= 2
    return out


def dot(a, b, dims=((1,), (0,))):
    return lax.dot_general(a, b, (dims, ((), ())), preferred_element_type=jnp.float32)


def wide(value):
    return value.astype(jnp.float32)


def narrow(value):
    return value.astype(jnp.bfloat16)


def padded(rows):
    return -(-rows // 16) * 16


def selection(count, rows, pad, flip=False):
    shape = (count * rows, count * pad) if flip else (count * pad, count * rows)
    long = lax.broadcasted_iota(jnp.int32, shape, 1 if flip else 0)
    short = lax.broadcasted_iota(jnp.int32, shape, 0 if flip else 1)
    piece = lax.shift_right_logical(long, jnp.int32(pad.bit_length() - 1))
    inner = long & (pad - 1)
    chosen = (short == piece * rows + inner) & (inner < rows)
    return narrow(jnp.where(chosen, 1.0, 0.0))


def slot_rows(ids, count):
    tokens = ids.shape[1]
    routed = jnp.max(jnp.where(ids == 0, 1.0, 0.0), axis=0, keepdims=True)
    spread = jnp.broadcast_to(routed, (count, tokens))
    row = lax.broadcasted_iota(jnp.int32, (tokens, tokens), 0)
    column = lax.broadcasted_iota(jnp.int32, (tokens, tokens), 1)
    upper = narrow(jnp.where(row <= column, 1.0, 0.0))
    rank = dot(narrow(spread), upper) - 1.0
    slot = wide(lax.broadcasted_iota(jnp.int32, (count, tokens), 0))
    return jnp.where((rank == slot) & (spread > 0.0), 1.0, 0.0)


class Links:
    def __init__(self, send_sems, recv_sems):
        self.send_sems = send_sems
        self.recv_sems = recv_sems
        self.count = 0
        self.sent = []

    def copy(self, src, dst, peer, axis="expert"):
        k = self.count
        self.count += 1
        assert k < SEMAPHORES
        return pltpu.make_async_remote_copy(
            src_ref=src,
            dst_ref=dst,
            send_sem=self.send_sems.at[k],
            recv_sem=self.recv_sems.at[k],
            device_id={axis: peer},
            device_id_type=MESH,
        )

    def start(self, copy):
        copy.start()
        self.sent.append(copy)


def layer_kernel(slices, chunks, rows, hop, *refs):
    inputs = 11 if hop else 7
    tok_f, tok_b, w_gate, w_up, w_down, pre_gate, pre_up = refs[:7]
    routes = refs[7:inputs]
    outs = 4 if hop else 3
    out_f, out_b, out_dots = refs[inputs : inputs + 3]
    (
        tok, wc, wd, gat_a, gat_b, par_a, par_b, xb, yb, pre, rs1, rs2, rsz, hold, hold2, zgot_b,
        sum_b, rs1_b, rs2_b, hold_b, sums, landed, table, table_got, dot_out, dot_in, local_sems,
        send_sems, recv_sems,
    ) = refs[inputs + outs :]
    device = lax.axis_index("expert")
    me = device % slices
    base = device - me
    lo = me % QUAD
    z = me // QUAD
    depth = slices // QUAD
    xp = base + xor(me, 1)
    yp = base + xor(me, 2)
    zp = [base + xor(z, q) * QUAD + lo for q in range(depth)]
    features, ff = wc.shape[0], wd.shape[0]
    width = features // chunks
    pad = padded(rows)
    cut = gat_a.shape[3]

    def bid(q, mask):
        return xor(z, q) * QUAD + xor(lo, mask)

    def cols_of(j):
        return pl.ds(j * width, width)

    loads = []

    def load(src, dst):
        copy = pltpu.make_async_copy(src, dst, local_sems.at[len(loads)])
        loads.append(copy)
        copy.start()
        return copy

    load_f = [load(tok_f.at[:, cols_of(j)], tok.at[0, :, cols_of(j)]) for j in range(chunks)]

    barrier = pltpu.get_barrier_semaphore()
    peers = [(q, m) for q in range(depth) for m in range(QUAD) if q or m]
    for q, m in peers:
        pl.semaphore_signal(
            barrier, inc=1, device_id={"expert": base + bid(q, m)}, device_id_type=MESH
        )
    greeted = len(peers)
    if hop:
        section = lax.axis_index("section")
        sections = lax.axis_size("section")
        ahead = (section + 1) % sections
        behind = (section + sections - 1) % sections
        for peer in (ahead, behind):
            pl.semaphore_signal(barrier, inc=1, device_id={"section": peer}, device_id_type=MESH)
        greeted += 2

    load_b, load_w = [], []

    def start_loads():
        for j in range(chunks):
            load_b.append(load(tok_b.at[:, cols_of(j)], tok.at[1, :, cols_of(j)]))
        for j in range(chunks):
            load_w.append(load(w_gate.at[cols_of(j), :], wc.at[cols_of(j), pl.ds(0, ff)]))
            load_w.append(load(w_up.at[cols_of(j), :], wc.at[cols_of(j), pl.ds(ff, ff)]))
            load_w.append(load(w_down.at[:, cols_of(j)], wd.at[:, cols_of(j)]))

    unpack = selection(chunks, rows, pad)
    pack = selection(chunks, rows, pad, flip=True)

    def choose(mb):
        if not hop:
            shape = (pad, tok.shape[1])
            same = lax.broadcasted_iota(jnp.int32, shape, 0)
            return narrow(
                jnp.where(same == lax.broadcasted_iota(jnp.int32, shape, 1), 1.0, 0.0)
            )
        ids = routes[2 * mb][...]
        return narrow(slot_rows(ids, pad))

    def send_tables():
        for mb in range(2):
            ids = routes[2 * mb][...]
            gates = jnp.where(ids == 0, routes[2 * mb + 1][...], 0.0)
            weighted = slot_rows(ids, LANES) * jnp.sum(gates, axis=0, keepdims=True)
            table[mb] = jnp.transpose(weighted)
            links.start(tables[mb])

    def place(mb, chosen, waits):
        for j in range(chunks):
            waits[j].wait()
            if mb == 0 and j == chunks - 1:
                start_loads()
            picked = dot(chosen, tok[mb, :, cols_of(j)])
            yb[0, pl.ds(j * pad, pad), :] = narrow(picked)
        packed = narrow(dot(pack, yb[0]))
        gat_a[mb, me] = packed[:, :cut]
        gat_b[mb, me] = packed[:, cut:]

    links = Links(send_sems, recv_sems)
    offsets = range(1, depth)
    own_x, own_y, forward, r1, r2 = {}, {}, {}, {}, {}
    zsend, rz, bsend, rb, dots_sent = {}, {}, {}, {}, {}
    for mb in range(2):
        for q in offsets:
            zsend[mb, q] = links.copy(gat_a.at[mb, me], gat_a.at[mb, me], zp[q])
            rz[mb, q] = links.copy(hold2.at[mb, q], rsz.at[mb, q], zp[q])
            quad = gat_b.at[mb, pl.ds(z * QUAD, QUAD)]
            bsend[mb, q] = links.copy(quad, quad, zp[q])
            theirs = par_b.at[mb, pl.ds(xor(z, q) * QUAD, QUAD)]
            rb[mb, q] = links.copy(theirs, zgot_b.at[mb, q], zp[q])
        for step in ["B"] + list(range(depth)):
            at = (mb, step)
            q, gat = (0, gat_b) if step == "B" else (step, gat_a)
            block = gat.at[mb, bid(q, 0)]
            own_x[at] = links.copy(block, block, xp)
            own_y[at] = links.copy(block, block, yp)
            via_x = GATHER_X[mb][step]
            got = gat.at[mb, bid(q, 2 if via_x else 1)]
            forward[at] = links.copy(got, got, xp if via_x else yp)
            m1, p1, p2 = (1, xp, yp) if REDUCE_X[mb][step] else (2, yp, xp)
            if step == "B":
                far, near = sum_b.at[mb, xor(lo, 3)], sum_b.at[mb, xor(lo, m1)]
                got1, held, got2 = rs1_b.at[mb], hold_b.at[mb], rs2_b.at[mb]
            else:
                far, near = par_a.at[mb, bid(q, 3)], par_a.at[mb, bid(q, m1)]
                got1, held, got2 = rs1.at[mb, q], hold.at[mb, q], rs2.at[mb, q]
            r1[at] = [links.copy(far, got1.at[1], p1), links.copy(near, got1.at[0], p1)]
            r2[at] = links.copy(held, got2, p2)
    for q in range(depth):
        dots_sent[q] = [
            links.copy(dot_out.at[bid(q, m)], dot_in.at[q * QUAD + m], base + bid(q, m))
            for m in range(QUAD)
            if q or m
        ]
    if hop:
        across = [
            links.copy(sums.at[0], landed.at[0], ahead, "section"),
            links.copy(sums.at[1], landed.at[1], behind, "section"),
        ]
        tables = [
            links.copy(table.at[0], table_got.at[0], ahead, "section"),
            links.copy(table.at[1], table_got.at[1], behind, "section"),
        ]

    arrived = []

    def await_all(*copies):
        for copy in copies:
            if not any(copy is done for done in arrived):
                arrived.append(copy)
                copy.wait_recv()

    def do_place(mb):
        place(mb, choose(mb), load_b if mb else load_f)
        if mb == 0:
            pl.semaphore_wait(barrier, greeted)

    def do_zs(mb, q):
        links.start(zsend[mb, q])

    def do_own(mb, step):
        if step != "B" and step > 0:
            await_all(zsend[mb, step])
        links.start(own_x[mb, step])
        links.start(own_y[mb, step])

    def do_fwd(mb, step):
        await_all((own_y if GATHER_X[mb][step] else own_x)[mb, step])
        links.start(forward[mb, step])

    def await_quad(mb, step):
        await_all(own_x[mb, step], own_y[mb, step], forward[mb, step])

    def do_bsend(mb, q):
        await_quad(mb, "B")
        links.start(bsend[mb, q])

    ready = []

    def do_compute(mb, q):
        await_quad(mb, q)
        if q > 0:
            await_all(bsend[mb, q])
        else:
            await_quad(mb, "B")
        if not ready:
            ready.append(True)
            for copy in load_w:
                copy.wait()
            spaced = selection(slices, rows, pad)
            for k, saved in enumerate((pre_gate, pre_up)):
                pre[k] = narrow(dot(spaced, saved[...])).reshape(pre.shape[1:])
        zq = xor(z, q)
        group = zq * QUAD
        for b in range(QUAD):
            full_a = narrow(dot(unpack, gat_a[mb, group + b]))
            full_b = narrow(dot(unpack, gat_b[mb, group + b]))
            for j in range(chunks):
                piece_rows = slice(j * pad, (j + 1) * pad)
                xb[pl.ds(b * pad, pad), pl.ds(j * width, cut)] = full_a[piece_rows]
                xb[pl.ds(b * pad, pad), pl.ds(j * width + cut, width - cut)] = full_b[piece_rows]
        total = None
        for j in range(chunks):
            if mb == 0:
                part = dot(xb[:, cols_of(j)], wc[cols_of(j), :])
            else:
                part = dot(xb[:, cols_of(j)], wd[:, cols_of(j)], ((1,), (1,)))
            total = part if total is None else total + part
        if mb == 0:
            gate = total[:, :ff]
            hidden = narrow(gate / (1.0 + jnp.exp(-gate)) * total[:, ff:])

            def piece(j):
                return dot(hidden, wd[:, cols_of(j)])

        else:
            gate = wide(pre[0, zq])
            up = wide(pre[1, zq])
            sig = 1.0 / (1.0 + jnp.exp(-gate))
            activated = gate * sig
            dots = jnp.sum(total * activated * up, axis=1, keepdims=True)
            for b in range(QUAD):
                mine = dots[b * pad : (b + 1) * pad]
                dot_out[group + b] = jnp.broadcast_to(mine, (pad, LANES))
            grad_gate = narrow(total * up * sig * (1.0 + gate * (1.0 - sig)))
            both = jnp.concatenate([grad_gate, narrow(total * activated)], axis=1)

            def piece(j):
                return dot(both, wc[cols_of(j), :], ((1,), (1,)))

        for j in range(chunks):
            full = narrow(piece(j))
            for b in range(QUAD):
                yb[b, pl.ds(j * pad, pad), :] = full[b * pad : (b + 1) * pad]
        for b in range(QUAD):
            packed = narrow(dot(pack, yb[b]))
            par_a[mb, group + b] = packed[:, :cut]
            par_b[mb, group + b] = packed[:, cut:]
        if q > 0:
            links.start(rb[mb, q])
        for copy in r1[mb, q]:
            links.start(copy)
        if mb == 1:
            for copy in dots_sent[q]:
                links.start(copy)

    def do_gather_b(mb):
        total = wide(par_b[mb, pl.ds(z * QUAD, QUAD)])
        for q in offsets:
            await_all(rb[mb, q])
            total = total + wide(zgot_b[mb, q])
        sum_b[mb] = narrow(total)
        for copy in r1[mb, "B"]:
            links.start(copy)

    def shares(mb, step):
        if step == "B":
            return (lambda m: sum_b[mb, xor(lo, m)]), rs1_b.at[mb], hold_b.at[mb], rs2_b.at[mb]
        q = step
        return (lambda m: par_a[mb, bid(q, m)]), rs1.at[mb, q], hold.at[mb, q], rs2.at[mb, q]

    def do_second(mb, step):
        mine, got, held, unused = shares(mb, step)
        await_all(r1[mb, step][0])
        held[...] = narrow(wide(mine(2 if REDUCE_X[mb][step] else 1)) + wide(got[1]))
        links.start(r2[mb, step])

    def do_third(mb, step):
        mine, got, unused, got2 = shares(mb, step)
        await_all(r1[mb, step][1], r2[mb, step])
        total = narrow(wide(mine(0)) + wide(got[0]) + wide(got2[...]))
        if step == "B":
            sums[mb, :, pl.ds(cut, width - cut)] = total
        else:
            hold2[mb, step] = total
            if step > 0:
                links.start(rz[mb, step])

    def do_finish(mb):
        total = wide(hold2[mb, 0])
        for q in offsets:
            await_all(rz[mb, q])
            total = total + wide(rsz[mb, q])
        sums[mb, :, pl.ds(0, cut)] = narrow(total)
        if hop:
            links.start(across[mb])

    def do_deliver(mb):
        out = (out_f, out_b)[mb]
        if mb == 1:
            found = dot_out[me]
            for q, m in peers:
                copy = links_to[q, m]
                await_all(copy)
                found = found + dot_in[q * QUAD + m]
            out_dots[...] = found
            if hop:
                out_tables = refs[inputs + 3]
                await_all(*tables)
                out_tables[...] = table_got[...]
        if hop:
            await_all(across[mb])
            out[...] = landed[mb]
        else:
            out[...] = sums[mb]

    links_to = {}
    for q in range(depth):
        masks = [m for m in range(QUAD) if q or m]
        for m, copy in zip(masks, dots_sent[q]):
            links_to[q, m] = copy

    events = {
        "place": do_place,
        "zs": do_zs,
        "own": do_own,
        "fwd": do_fwd,
        "zB": do_bsend,
        "comp": do_compute,
        "sumB": do_gather_b,
        "sec": do_second,
        "thi": do_third,
        "fin": do_finish,
        "del": do_deliver,
    }
    for entry in SCHEDULE:
        event, *at = entry.split()
        events[event](*(step if step == "B" else int(step) for step in at))
        if entry == TABLES_AFTER and hop:
            send_tables()
    for copy in links.sent:
        copy.wait_send()


def run_layer(tok_f, tok_b, w_gate, w_up, w_down, pre_gate, pre_up, routes, slices, rows):
    hop = bool(routes)
    features = tok_f.shape[1]
    chunks = 16 // math.gcd(16, rows)
    width = features // chunks
    ff = w_gate.shape[1]
    depth = slices // QUAD
    pad = padded(rows)
    group = QUAD * pad

    vmem = pl.BlockSpec(memory_space=pltpu.VMEM)
    anywhere = pl.BlockSpec(memory_space=pl.ANY)
    block = (chunks * rows, width)
    last = max(width // LANES // 7, 1) * LANES
    part_a, part_b = (chunks * rows, width - last), (chunks * rows, last)
    tables = (2, tok_f.shape[0] if hop else 8, LANES)
    out_shape = [
        jax.ShapeDtypeStruct(block, jnp.bfloat16),
        jax.ShapeDtypeStruct(block, jnp.bfloat16),
        jax.ShapeDtypeStruct((pad, LANES), jnp.float32),
    ]
    if hop:
        out_shape.append(jax.ShapeDtypeStruct(tables, jnp.float32))
    return pl.pallas_call(
        functools.partial(layer_kernel, slices, chunks, rows, hop),
        out_shape=tuple(out_shape),
        in_specs=[anywhere] * 5 + [vmem] * (2 + len(routes)),
        out_specs=(vmem,) * len(out_shape),
        scratch_shapes=[
            pltpu.VMEM((2,) + tok_f.shape, jnp.bfloat16),
            pltpu.VMEM((features, 2 * ff), jnp.bfloat16),
            pltpu.VMEM((ff, features), jnp.bfloat16),
            pltpu.VMEM((2, slices) + part_a, jnp.bfloat16),
            pltpu.VMEM((2, slices) + part_b, jnp.bfloat16),
            pltpu.VMEM((2, slices) + part_a, jnp.bfloat16),
            pltpu.VMEM((2, slices) + part_b, jnp.bfloat16),
            pltpu.VMEM((group, features), jnp.bfloat16),
            pltpu.VMEM((QUAD, chunks * pad, width), jnp.bfloat16),
            pltpu.VMEM((2, depth, group, ff), jnp.bfloat16),
            pltpu.VMEM((2, depth, 2) + part_a, jnp.bfloat16),
            pltpu.VMEM((2, depth) + part_a, jnp.bfloat16),
            pltpu.VMEM((2, depth) + part_a, jnp.bfloat16),
            pltpu.VMEM((2, depth) + part_a, jnp.bfloat16),
            pltpu.VMEM((2, depth) + part_a, jnp.bfloat16),
            pltpu.VMEM((2, depth, QUAD) + part_b, jnp.bfloat16),
            pltpu.VMEM((2, QUAD) + part_b, jnp.bfloat16),
            pltpu.VMEM((2, 2) + part_b, jnp.bfloat16),
            pltpu.VMEM((2,) + part_b, jnp.bfloat16),
            pltpu.VMEM((2,) + part_b, jnp.bfloat16),
            pltpu.VMEM((2,) + block, jnp.bfloat16),
            pltpu.VMEM((2,) + block, jnp.bfloat16),
            pltpu.VMEM(tables, jnp.float32),
            pltpu.VMEM(tables, jnp.float32),
            pltpu.VMEM((slices, pad, LANES), jnp.float32),
            pltpu.VMEM((slices, pad, LANES), jnp.float32),
            pltpu.SemaphoreType.DMA((5 * chunks,)),
            pltpu.SemaphoreType.DMA((SEMAPHORES,)),
            pltpu.SemaphoreType.DMA((SEMAPHORES,)),
        ],
        compiler_params=pltpu.CompilerParams(
            collective_id=0, has_side_effects=True, vmem_limit_bytes=56 * 2**20
        ),
        name="moe_layer",
    )(tok_f, tok_b, w_gate, w_up, w_down, pre_gate, pre_up, *routes)


def mix_kernel(rows, graded, *refs):
    block_f, block_b, tables = refs[:3]
    extra = 2 if graded else 0
    outs = refs[3 + extra : 5 + extra]
    stage, sems = refs[-2:]
    block_rows, width = block_f.shape
    chunks = block_rows // rows
    pad = padded(rows)
    unpack = selection(chunks, rows, pad)
    copies = []
    for k, block in enumerate((block_f, block_b)):
        weight = tables[k][:, :pad]
        high = narrow(weight)
        both = jnp.concatenate([high, narrow(weight - wide(high))], axis=1)
        full = narrow(dot(unpack, block[...]))
        for j in range(chunks):
            part = full[j * pad : (j + 1) * pad]
            cols = pl.ds(j * width, width)
            stage[k, :, cols] = narrow(dot(both, jnp.concatenate([part, part], axis=0)))
            copies.append(
                pltpu.make_async_copy(
                    stage.at[k, :, cols], outs[k].at[:, cols], sems.at[k * chunks + j]
                )
            )
            copies[-1].start()
    if graded:
        dots, ids = refs[3], refs[4]
        slots = slot_rows(ids[...], pad)
        found = jnp.sum(slots * dots[...], axis=0, keepdims=True)
        refs[7][...] = jnp.where(ids[...] == 0, found, 0.0)
    for copy in copies:
        copy.wait()


def mix(block_f, block_b, tables, rows, grading):
    block_rows, width = block_f.shape
    tokens = tables.shape[1]
    chunks = block_rows // rows
    vmem = pl.BlockSpec(memory_space=pltpu.VMEM)
    anywhere = pl.BlockSpec(memory_space=pl.ANY)
    shape = jax.ShapeDtypeStruct((tokens, chunks * width), jnp.bfloat16)
    out_shape = [shape, shape]
    if grading:
        out_shape.append(jax.ShapeDtypeStruct(grading[1].shape, jnp.float32))
    return pl.pallas_call(
        functools.partial(mix_kernel, rows, bool(grading)),
        out_shape=tuple(out_shape),
        in_specs=[vmem] * (3 + len(grading)),
        out_specs=tuple([anywhere, anywhere] + [vmem] * (len(out_shape) - 2)),
        scratch_shapes=[
            pltpu.VMEM((2, tokens, chunks * width), jnp.bfloat16),
            pltpu.SemaphoreType.DMA((2 * chunks,)),
        ],
        name="mix",
    )(block_f, block_b, tables, *grading)


def body(
    act_in,
    cotangent,
    fwd_ids,
    fwd_gates,
    bwd_ids,
    bwd_gates,
    gate_w,
    up_w,
    down_w,
    gate_pre,
    up_pre,
):
    ndev = lax.axis_size("expert")
    ff_dev = gate_w.shape[2]
    slices = FF // ff_dev
    experts = ndev // slices
    capacity = gate_pre.shape[1] // ndev
    rows = experts * capacity
    weights = (gate_w[0], up_w[0], down_w[0])

    if experts == 1:
        routes = tuple(each[0].T for each in (fwd_ids, fwd_gates, bwd_ids, bwd_gates))
        block_f, block_b, dots, tables = run_layer(
            act_in[0], cotangent[0], *weights, gate_pre[0], up_pre[0], routes, slices, rows
        )
        next_act, prev_grad, grads = mix(block_f, block_b, tables, rows, (dots, routes[2]))
        return (next_act[None], prev_grad[None], grads.T[None])

    chunks = 16 // math.gcd(16, rows)
    features = act_in.shape[2]
    width = features // chunks
    columns = [[g * slices + i for g in range(experts)] for i in range(slices)]

    def exchange(value):
        return lax.all_to_all(
            value, "expert", split_axis=0, concat_axis=0, axis_index_groups=columns, tiled=True
        )

    matches_f, placing_f, weights_f = routing(fwd_ids[0], fwd_gates[0], experts, capacity)
    matches_b, placing_b, weights_b = routing(bwd_ids[0], bwd_gates[0], experts, capacity)

    def prepare(tokens, placing):
        chosen = placing.reshape(rows, tokens.shape[0])
        picked = dot(chosen.astype(jnp.bfloat16), tokens).astype(jnp.bfloat16)
        picked = exchange(picked.reshape(experts, capacity, features))
        return picked.reshape(rows, features)

    def by_group(saved):
        saved = saved.reshape(experts, slices, capacity, ff_dev).transpose(1, 0, 2, 3)
        return saved.reshape(slices * rows, ff_dev)

    block_f, block_b, dots = run_layer(
        prepare(act_in[0], placing_f), prepare(cotangent[0], placing_b), *weights,
        by_group(gate_pre[0]), by_group(up_pre[0]), (), slices, rows,
    )
    mine = exchange(dots[:rows, 0].reshape(experts, capacity))

    def send_back(block):
        table = block.reshape(chunks, rows, width).transpose(1, 0, 2)
        table = exchange(table.reshape(experts, capacity, features))
        table = table.reshape(rows, chunks, width).transpose(1, 0, 2)
        return table.reshape(chunks * rows, width)

    token_dots = jnp.sum(placing_b * mine[:, :, None], axis=1)
    gate_grad = jnp.sum(jnp.where(matches_b, token_dots[:, :, None], 0.0), axis=0)

    def weight_table(placing, weights):
        table = (placing * weights[:, None, :]).reshape(rows, -1).T
        return jnp.pad(table, ((0, 0), (0, LANES - rows)))

    def onward(block, placing, weights, step):
        block = from_behind(send_back(block), "section", step)
        return block, from_behind(weight_table(placing, weights), "section", step)

    block_f, table_f = onward(block_f, placing_f, weights_f, 1)
    block_b, table_b = onward(block_b, placing_b, weights_b, -1)
    next_act, prev_grad = mix(block_f, block_b, jnp.stack([table_f, table_b]), rows, ())
    return (next_act[None], prev_grad[None], gate_grad[None])


def solution(mesh):
    in_specs = (
        P("section", "expert", None),
        P("section", "expert", None),
        P("section", "expert", None),
        P("section", "expert", None),
        P("section", "expert", None),
        P("section", "expert", None),
        P("section", None, "expert"),
        P("section", None, "expert"),
        P("section", "expert", None),
        P("section", None, "expert"),
        P("section", None, "expert"),
    )
    out_specs = (
        P("section", "expert", None),
        P("section", "expert", None),
        P("section", "expert", None),
    )
    return jax.shard_map(body, mesh=mesh, in_specs=in_specs, out_specs=out_specs, check_vma=False)
```

```python
import functools
import math

import jax
import jax.numpy as jnp
from jax import lax
from jax.experimental import pallas as pl
from jax.experimental.pallas import tpu as pltpu
from jax.sharding import PartitionSpec as P

FF = 2048
QUAD = 4
LANES = 128
SEMAPHORES = 160
TABLES_AFTER = "fwd 0 B"
MESH = pl.DeviceIdType.MESH

SCHEDULE = (
    "place 0", "oy 0 B", "ox 0 0", "zs 0 2", "zs 0 1", "place 1", "oy 1 0", "zs 1 2", "ox 0 B",
    "oy 1 B", "ox 1 0", "oy 0 0", "zs 1 1", "fwd 0 0", "ox 1 B", "fwd 0 B", "fwd 1 0",
    "fwd 1 B", "ox 0 1", "oy 0 2", "oy 0 1", "zs 0 3", "ox 0 2", "zB 0 1", "comp 0 0", "zB 1 1",
    "ox 1 1", "oy 1 2", "ox 1 2", "comp 1 0", "fwd 0 2", "zB 0 2", "fwd 1 2", "oy 0 3",
    "fwd 0 1", "zB 1 2", "ox 0 3", "oy 1 1", "zB 0 3", "zs 1 3", "fwd 1 1", "comp 0 2",
    "rf 0 2", "zB 1 3", "fwd 0 3", "rn 0 2", "comp 1 2", "rb 0 2", "rf 1 2", "rb 1 2",
    "comp 0 1", "oy 1 3", "ox 1 3", "comp 1 1", "rn 1 2", "sec 1 2", "comp 0 3", "rb 0 3",
    "rf 0 3", "fwd 1 3", "sec 0 2", "rf 0 1", "rn 0 1", "rn 0 3", "rb 0 1", "thi 1 2", "rz 1 2",
    "rb 1 1", "comp 1 3", "rf 1 3", "sec 0 3", "sec 0 1", "rb 1 3", "rn 1 3", "sumB 0",
    "rf 1 1", "thi 0 2", "rz 0 2", "thi 0 3", "rz 0 3", "sec 1 3", "rn 1 1", "sec 0 B",
    "rf 1 0", "rf 0 0", "thi 0 1", "rz 0 1", "sec 1 1", "thi 1 3", "sumB 1", "rz 1 3", "rn 0 0",
    "thi 0 B", "rn 1 0", "sec 0 0", "thi 1 1", "rz 1 1", "sec 1 0", "sec 1 B", "thi 0 0",
    "fin 0", "thi 1 0", "thi 1 B", "fin 1", "del 0", "del 1",
)
GATHER_X = (
    {"B": True, 0: False, 1: True, 2: False, 3: True},
    {"B": True, 0: True, 1: False, 2: True, 3: False},
)
REDUCE_X = (
    {"B": False, 0: True, 1: False, 2: False, 3: True},
    {"B": True, 0: False, 1: False, 2: True, 3: True},
)


def from_behind(value, axis, steps):
    count = lax.axis_size(axis)
    pairs = [(source, (source + steps) % count) for source in range(count)]
    return lax.ppermute(value, axis, pairs)


def routing(ids, gates, experts, capacity):
    expert_ids = jnp.arange(experts, dtype=jnp.int32)
    matches = ids[None, :, :] == expert_ids[:, None, None]
    routed = jnp.any(matches, axis=2)
    weights = jnp.sum(jnp.where(matches, gates[None, :, :], 0.0), axis=2)
    tokens = ids.shape[0]
    earlier = jnp.arange(tokens)[:, None] <= jnp.arange(tokens)[None, :]
    counted = jnp.sum(jnp.where(routed[:, :, None] & earlier[None], 1, 0), axis=1)
    position = counted - 1
    slot_ids = jnp.arange(capacity, dtype=jnp.int32)
    placing = (position[:, None, :] == slot_ids[None, :, None]) & routed[:, None, :]
    return (matches, placing.astype(jnp.float32), weights)


def xor(value, mask):
    out = value
    bit = 1
    while bit <= mask:
        if mask & bit:
            out = out + bit - 2 * bit * ((value // bit) % 2)
        bit *= 2
    return out


def dot(a, b, dims=((1,), (0,))):
    return lax.dot_general(a, b, (dims, ((), ())), preferred_element_type=jnp.float32)


def wide(value):
    return value.astype(jnp.float32)


def narrow(value):
    return value.astype(jnp.bfloat16)


def padded(rows):
    return -(-rows // 16) * 16


def selection(count, rows, pad, flip=False):
    shape = (count * rows, count * pad) if flip else (count * pad, count * rows)
    long = lax.broadcasted_iota(jnp.int32, shape, 1 if flip else 0)
    short = lax.broadcasted_iota(jnp.int32, shape, 0 if flip else 1)
    piece = lax.shift_right_logical(long, jnp.int32(pad.bit_length() - 1))
    inner = long & (pad - 1)
    chosen = (short == piece * rows + inner) & (inner < rows)
    return narrow(jnp.where(chosen, 1.0, 0.0))


def slot_rows(ids, count):
    tokens = ids.shape[1]
    routed = jnp.max(jnp.where(ids == 0, 1.0, 0.0), axis=0, keepdims=True)
    spread = jnp.broadcast_to(routed, (count, tokens))
    row = lax.broadcasted_iota(jnp.int32, (tokens, tokens), 0)
    column = lax.broadcasted_iota(jnp.int32, (tokens, tokens), 1)
    upper = narrow(jnp.where(row <= column, 1.0, 0.0))
    rank = dot(narrow(spread), upper) - 1.0
    slot = wide(lax.broadcasted_iota(jnp.int32, (count, tokens), 0))
    return jnp.where((rank == slot) & (spread > 0.0), 1.0, 0.0)


class Links:
    def __init__(self, send_sems, recv_sems):
        self.send_sems = send_sems
        self.recv_sems = recv_sems
        self.count = 0
        self.sent = []

    def copy(self, src, dst, peer, axis="expert"):
        k = self.count
        self.count += 1
        assert k < SEMAPHORES
        return pltpu.make_async_remote_copy(
            src_ref=src,
            dst_ref=dst,
            send_sem=self.send_sems.at[k],
            recv_sem=self.recv_sems.at[k],
            device_id={axis: peer},
            device_id_type=MESH,
        )

    def start(self, copy):
        copy.start()
        self.sent.append(copy)


def layer_kernel(slices, chunks, rows, hop, *refs):
    inputs = 11 if hop else 7
    tok_f, tok_b, w_gate, w_up, w_down, pre_gate, pre_up = refs[:7]
    routes = refs[7:inputs]
    outs = 4 if hop else 3
    out_f, out_b, out_dots = refs[inputs : inputs + 3]
    (
        tok, wc, wd, gat_a, gat_b, par_a, par_b, xb, yb, pre, rs1, rs2, rsz, hold, hold2, zgot_b,
        sum_b, rs1_b, rs2_b, hold_b, sums, landed, table, table_got, dot_out, dot_in, local_sems,
        send_sems, recv_sems,
    ) = refs[inputs + outs :]
    device = lax.axis_index("expert")
    me = device % slices
    base = device - me
    lo = me % QUAD
    z = me // QUAD
    depth = slices // QUAD
    xp = base + xor(me, 1)
    yp = base + xor(me, 2)
    zp = [base + xor(z, q) * QUAD + lo for q in range(depth)]
    features, ff = wc.shape[0], wd.shape[0]
    width = features // chunks
    pad = padded(rows)
    cut = gat_a.shape[3]

    def bid(q, mask):
        return xor(z, q) * QUAD + xor(lo, mask)

    def cols_of(j):
        return pl.ds(j * width, width)

    loads = []

    def load(src, dst):
        copy = pltpu.make_async_copy(src, dst, local_sems.at[len(loads)])
        loads.append(copy)
        copy.start()
        return copy

    load_f = [load(tok_f.at[:, cols_of(j)], tok.at[0, :, cols_of(j)]) for j in range(chunks)]

    barrier = pltpu.get_barrier_semaphore()
    peers = [(q, m) for q in range(depth) for m in range(QUAD) if q or m]
    for q, m in peers:
        pl.semaphore_signal(
            barrier, inc=1, device_id={"expert": base + bid(q, m)}, device_id_type=MESH
        )
    greeted = len(peers)
    if hop:
        section = lax.axis_index("section")
        sections = lax.axis_size("section")
        ahead = (section + 1) % sections
        behind = (section + sections - 1) % sections
        for peer in (ahead, behind):
            pl.semaphore_signal(barrier, inc=1, device_id={"section": peer}, device_id_type=MESH)
        greeted += 2

    load_b, load_w = [], []

    def start_loads():
        for j in range(chunks):
            load_b.append(load(tok_b.at[:, cols_of(j)], tok.at[1, :, cols_of(j)]))
        for j in range(chunks):
            load_w.append(load(w_gate.at[cols_of(j), :], wc.at[cols_of(j), pl.ds(0, ff)]))
            load_w.append(load(w_up.at[cols_of(j), :], wc.at[cols_of(j), pl.ds(ff, ff)]))
            load_w.append(load(w_down.at[:, cols_of(j)], wd.at[:, cols_of(j)]))

    unpack = selection(chunks, rows, pad)
    pack = selection(chunks, rows, pad, flip=True)

    def choose(mb):
        if not hop:
            shape = (pad, tok.shape[1])
            same = lax.broadcasted_iota(jnp.int32, shape, 0)
            return narrow(
                jnp.where(same == lax.broadcasted_iota(jnp.int32, shape, 1), 1.0, 0.0)
            )
        ids = routes[2 * mb][...]
        return narrow(slot_rows(ids, pad))

    def send_tables():
        for mb in range(2):
            ids = routes[2 * mb][...]
            gates = jnp.where(ids == 0, routes[2 * mb + 1][...], 0.0)
            weighted = slot_rows(ids, LANES) * jnp.sum(gates, axis=0, keepdims=True)
            table[mb] = jnp.transpose(weighted)
            links.start(tables[mb])

    def place(mb, chosen, waits):
        for j in range(chunks):
            waits[j].wait()
            if mb == 0 and j == chunks - 1:
                start_loads()
            picked = dot(chosen, tok[mb, :, cols_of(j)])
            yb[0, pl.ds(j * pad, pad), :] = narrow(picked)
        packed = narrow(dot(pack, yb[0]))
        gat_a[mb, me] = packed[:, :cut]
        gat_b[mb, me] = packed[:, cut:]

    links = Links(send_sems, recv_sems)
    offsets = range(1, depth)
    own_x, own_y, forward, r1, r2 = {}, {}, {}, {}, {}
    zsend, rz, bsend, rb, dots_sent = {}, {}, {}, {}, {}
    for mb in range(2):
        for q in offsets:
            zsend[mb, q] = links.copy(gat_a.at[mb, me], gat_a.at[mb, me], zp[q])
            rz[mb, q] = links.copy(hold2.at[mb, q], rsz.at[mb, q], zp[q])
            for up in (1, -1):
                source = jnp.clip(z - up * (q - 1), 0, depth - 1)
                quad = gat_b.at[mb, pl.ds(source * QUAD, QUAD)]
                peer = base + jnp.clip(z + up, 0, depth - 1) * QUAD + lo
                bsend[mb, q, up] = links.copy(quad, quad, peer)
            theirs = par_b.at[mb, pl.ds(xor(z, q) * QUAD, QUAD)]
            rb[mb, q] = links.copy(theirs, zgot_b.at[mb, q], zp[q])
        for step in ["B"] + list(range(depth)):
            at = (mb, step)
            q, gat = (0, gat_b) if step == "B" else (step, gat_a)
            block = gat.at[mb, bid(q, 0)]
            own_x[at] = links.copy(block, block, xp)
            own_y[at] = links.copy(block, block, yp)
            via_x = GATHER_X[mb][step]
            got = gat.at[mb, bid(q, 2 if via_x else 1)]
            forward[at] = links.copy(got, got, xp if via_x else yp)
            m1, p1, p2 = (1, xp, yp) if REDUCE_X[mb][step] else (2, yp, xp)
            if step == "B":
                far, near = sum_b.at[mb, xor(lo, 3)], sum_b.at[mb, xor(lo, m1)]
                got1, held, got2 = rs1_b.at[mb], hold_b.at[mb], rs2_b.at[mb]
            else:
                far, near = par_a.at[mb, bid(q, 3)], par_a.at[mb, bid(q, m1)]
                got1, held, got2 = rs1.at[mb, q], hold.at[mb, q], rs2.at[mb, q]
            r1[at] = [links.copy(far, got1.at[1], p1), links.copy(near, got1.at[0], p1)]
            r2[at] = links.copy(held, got2, p2)
    for q in range(depth):
        dots_sent[q] = [
            links.copy(dot_out.at[bid(q, m)], dot_in.at[q * QUAD + m], base + bid(q, m))
            for m in range(QUAD)
            if q or m
        ]
    if hop:
        across = [
            links.copy(sums.at[0], landed.at[0], ahead, "section"),
            links.copy(sums.at[1], landed.at[1], behind, "section"),
        ]
        tables = [
            links.copy(table.at[0], table_got.at[0], ahead, "section"),
            links.copy(table.at[1], table_got.at[1], behind, "section"),
        ]

    arrived = []

    def await_all(*copies):
        for copy in copies:
            if not any(copy is done for done in arrived):
                arrived.append(copy)
                copy.wait_recv()

    def do_place(mb):
        place(mb, choose(mb), load_b if mb else load_f)
        if mb == 0:
            pl.semaphore_wait(barrier, greeted)

    def do_zs(mb, q):
        links.start(zsend[mb, q])

    def do_own(mb, step, copies):
        if step != "B" and step > 0:
            await_all(zsend[mb, step])
        links.start(copies[mb, step])

    def do_fwd(mb, step):
        await_all((own_y if GATHER_X[mb][step] else own_x)[mb, step])
        links.start(forward[mb, step])

    def await_quad(mb, step):
        await_all(own_x[mb, step], own_y[mb, step], forward[mb, step])

    def do_bsend(mb, hop):
        if hop == 1:
            await_quad(mb, "B")
        for up in (1, -1):
            source, onward = z - up * (hop - 1), z + up
            held = (source >= 0) & (source < depth)
            if hop > 1:

                @pl.when(held)
                def _():
                    bsend[mb, hop - 1, up].wait_recv()

            @pl.when(held & (onward >= 0) & (onward < depth))
            def _():
                bsend[mb, hop, up].start()

    def finish_bsend(mb):
        for hop in range(1, depth):
            for up in (1, -1):
                source, onward = z - up * (hop - 1), z + up
                held = (source >= 0) & (source < depth)

                @pl.when(held & (onward >= 0) & (onward < depth))
                def _():
                    bsend[mb, hop, up].wait_send()

    ended = []

    def last_hop(mb):
        if mb not in ended:
            ended.append(mb)
            for up in (1, -1):
                source = z - up * (depth - 1)

                @pl.when((source >= 0) & (source < depth))
                def _():
                    bsend[mb, depth - 1, up].wait_recv()

    ready = []

    def do_compute(mb, q):
        await_quad(mb, q)
        if q == 0:
            await_quad(mb, "B")
        elif q == depth - 1:
            last_hop(mb)
        if not ready:
            ready.append(True)
            for copy in load_w:
                copy.wait()
            spaced = selection(slices, rows, pad)
            for k, saved in enumerate((pre_gate, pre_up)):
                pre[k] = narrow(dot(spaced, saved[...])).reshape(pre.shape[1:])
        zq = xor(z, q)
        group = zq * QUAD
        for b in range(QUAD):
            full_a = narrow(dot(unpack, gat_a[mb, group + b]))
            full_b = narrow(dot(unpack, gat_b[mb, group + b]))
            for j in range(chunks):
                piece_rows = slice(j * pad, (j + 1) * pad)
                xb[pl.ds(b * pad, pad), pl.ds(j * width, cut)] = full_a[piece_rows]
                xb[pl.ds(b * pad, pad), pl.ds(j * width + cut, width - cut)] = full_b[piece_rows]
        total = None
        for j in range(chunks):
            if mb == 0:
                part = dot(xb[:, cols_of(j)], wc[cols_of(j), :])
            else:
                part = dot(xb[:, cols_of(j)], wd[:, cols_of(j)], ((1,), (1,)))
            total = part if total is None else total + part
        if mb == 0:
            gate = total[:, :ff]
            hidden = narrow(gate / (1.0 + jnp.exp(-gate)) * total[:, ff:])

            def piece(j):
                return dot(hidden, wd[:, cols_of(j)])

        else:
            gate = wide(pre[0, zq])
            up = wide(pre[1, zq])
            sig = 1.0 / (1.0 + jnp.exp(-gate))
            activated = gate * sig
            dots = jnp.sum(total * activated * up, axis=1, keepdims=True)
            for b in range(QUAD):
                mine = dots[b * pad : (b + 1) * pad]
                dot_out[group + b] = jnp.broadcast_to(mine, (pad, LANES))
            grad_gate = narrow(total * up * sig * (1.0 + gate * (1.0 - sig)))
            both = jnp.concatenate([grad_gate, narrow(total * activated)], axis=1)

            def piece(j):
                return dot(both, wc[cols_of(j), :], ((1,), (1,)))

        for j in range(chunks):
            full = narrow(piece(j))
            for b in range(QUAD):
                yb[b, pl.ds(j * pad, pad), :] = full[b * pad : (b + 1) * pad]
        for b in range(QUAD):
            packed = narrow(dot(pack, yb[b]))
            par_a[mb, group + b] = packed[:, :cut]
            par_b[mb, group + b] = packed[:, cut:]
        if mb == 1:
            for copy in dots_sent[q]:
                links.start(copy)

    def do_gather_b(mb):
        total = wide(par_b[mb, pl.ds(z * QUAD, QUAD)])
        for q in offsets:
            await_all(rb[mb, q])
            total = total + wide(zgot_b[mb, q])
        sum_b[mb] = narrow(total)
        for copy in r1[mb, "B"]:
            links.start(copy)

    def shares(mb, step):
        if step == "B":
            return (lambda m: sum_b[mb, xor(lo, m)]), rs1_b.at[mb], hold_b.at[mb], rs2_b.at[mb]
        q = step
        return (lambda m: par_a[mb, bid(q, m)]), rs1.at[mb, q], hold.at[mb, q], rs2.at[mb, q]

    def do_second(mb, step):
        mine, got, held, unused = shares(mb, step)
        await_all(r1[mb, step][0])
        held[...] = narrow(wide(mine(2 if REDUCE_X[mb][step] else 1)) + wide(got[1]))
        links.start(r2[mb, step])

    def do_third(mb, step):
        mine, got, unused, got2 = shares(mb, step)
        await_all(r1[mb, step][1], r2[mb, step])
        total = narrow(wide(mine(0)) + wide(got[0]) + wide(got2[...]))
        if step == "B":
            sums[mb, :, pl.ds(cut, width - cut)] = total
        else:
            hold2[mb, step] = total

    def do_finish(mb):
        total = wide(hold2[mb, 0])
        for q in offsets:
            await_all(rz[mb, q])
            total = total + wide(rsz[mb, q])
        sums[mb, :, pl.ds(0, cut)] = narrow(total)
        if hop:
            links.start(across[mb])

    def do_deliver(mb):
        out = (out_f, out_b)[mb]
        if mb == 1:
            found = dot_out[me]
            for q, m in peers:
                copy = links_to[q, m]
                await_all(copy)
                found = found + dot_in[q * QUAD + m]
            out_dots[...] = found
            if hop:
                out_tables = refs[inputs + 3]
                await_all(*tables)
                out_tables[...] = table_got[...]
        if hop:
            await_all(across[mb])
            out[...] = landed[mb]
        else:
            out[...] = sums[mb]

    links_to = {}
    for q in range(depth):
        masks = [m for m in range(QUAD) if q or m]
        for m, copy in zip(masks, dots_sent[q]):
            links_to[q, m] = copy

    events = {
        "place": do_place,
        "zs": do_zs,
        "ox": lambda mb, step: do_own(mb, step, own_x),
        "oy": lambda mb, step: do_own(mb, step, own_y),
        "fwd": do_fwd,
        "zB": do_bsend,
        "comp": do_compute,
        "rb": lambda mb, q: links.start(rb[mb, q]),
        "rf": lambda mb, q: links.start(r1[mb, q][0]),
        "rn": lambda mb, q: links.start(r1[mb, q][1]),
        "rz": lambda mb, q: links.start(rz[mb, q]),
        "sumB": do_gather_b,
        "sec": do_second,
        "thi": do_third,
        "fin": do_finish,
        "del": do_deliver,
    }
    for entry in SCHEDULE:
        event, *at = entry.split()
        events[event](*(step if step == "B" else int(step) for step in at))
        if entry == TABLES_AFTER and hop:
            send_tables()
    for mb in range(2):
        finish_bsend(mb)
    for copy in links.sent:
        copy.wait_send()


def run_layer(tok_f, tok_b, w_gate, w_up, w_down, pre_gate, pre_up, routes, slices, rows):
    hop = bool(routes)
    features = tok_f.shape[1]
    chunks = 16 // math.gcd(16, rows)
    width = features // chunks
    ff = w_gate.shape[1]
    depth = slices // QUAD
    pad = padded(rows)
    group = QUAD * pad

    vmem = pl.BlockSpec(memory_space=pltpu.VMEM)
    anywhere = pl.BlockSpec(memory_space=pl.ANY)
    block = (chunks * rows, width)
    last = max(width // LANES // 7, 1) * LANES
    part_a, part_b = (chunks * rows, width - last), (chunks * rows, last)
    tables = (2, tok_f.shape[0] if hop else 8, LANES)
    out_shape = [
        jax.ShapeDtypeStruct(block, jnp.bfloat16),
        jax.ShapeDtypeStruct(block, jnp.bfloat16),
        jax.ShapeDtypeStruct((pad, LANES), jnp.float32),
    ]
    if hop:
        out_shape.append(jax.ShapeDtypeStruct(tables, jnp.float32))
    return pl.pallas_call(
        functools.partial(layer_kernel, slices, chunks, rows, hop),
        out_shape=tuple(out_shape),
        in_specs=[anywhere] * 5 + [vmem] * (2 + len(routes)),
        out_specs=(vmem,) * len(out_shape),
        scratch_shapes=[
            pltpu.VMEM((2,) + tok_f.shape, jnp.bfloat16),
            pltpu.VMEM((features, 2 * ff), jnp.bfloat16),
            pltpu.VMEM((ff, features), jnp.bfloat16),
            pltpu.VMEM((2, slices) + part_a, jnp.bfloat16),
            pltpu.VMEM((2, slices) + part_b, jnp.bfloat16),
            pltpu.VMEM((2, slices) + part_a, jnp.bfloat16),
            pltpu.VMEM((2, slices) + part_b, jnp.bfloat16),
            pltpu.VMEM((group, features), jnp.bfloat16),
            pltpu.VMEM((QUAD, chunks * pad, width), jnp.bfloat16),
            pltpu.VMEM((2, depth, group, ff), jnp.bfloat16),
            pltpu.VMEM((2, depth, 2) + part_a, jnp.bfloat16),
            pltpu.VMEM((2, depth) + part_a, jnp.bfloat16),
            pltpu.VMEM((2, depth) + part_a, jnp.bfloat16),
            pltpu.VMEM((2, depth) + part_a, jnp.bfloat16),
            pltpu.VMEM((2, depth) + part_a, jnp.bfloat16),
            pltpu.VMEM((2, depth, QUAD) + part_b, jnp.bfloat16),
            pltpu.VMEM((2, QUAD) + part_b, jnp.bfloat16),
            pltpu.VMEM((2, 2) + part_b, jnp.bfloat16),
            pltpu.VMEM((2,) + part_b, jnp.bfloat16),
            pltpu.VMEM((2,) + part_b, jnp.bfloat16),
            pltpu.VMEM((2,) + block, jnp.bfloat16),
            pltpu.VMEM((2,) + block, jnp.bfloat16),
            pltpu.VMEM(tables, jnp.float32),
            pltpu.VMEM(tables, jnp.float32),
            pltpu.VMEM((slices, pad, LANES), jnp.float32),
            pltpu.VMEM((slices, pad, LANES), jnp.float32),
            pltpu.SemaphoreType.DMA((5 * chunks,)),
            pltpu.SemaphoreType.DMA((SEMAPHORES,)),
            pltpu.SemaphoreType.DMA((SEMAPHORES,)),
        ],
        compiler_params=pltpu.CompilerParams(
            collective_id=0, has_side_effects=True, vmem_limit_bytes=56 * 2**20
        ),
        name="moe_layer",
    )(tok_f, tok_b, w_gate, w_up, w_down, pre_gate, pre_up, *routes)


def mix_kernel(rows, graded, *refs):
    block_f, block_b, tables = refs[:3]
    extra = 2 if graded else 0
    outs = refs[3 + extra : 5 + extra]
    stage, sems = refs[-2:]
    block_rows, width = block_f.shape
    chunks = block_rows // rows
    pad = padded(rows)
    unpack = selection(chunks, rows, pad)
    copies = []
    for k, block in enumerate((block_f, block_b)):
        weight = tables[k][:, :pad]
        high = narrow(weight)
        both = jnp.concatenate([high, narrow(weight - wide(high))], axis=1)
        full = narrow(dot(unpack, block[...]))
        for j in range(chunks):
            part = full[j * pad : (j + 1) * pad]
            cols = pl.ds(j * width, width)
            stage[k, :, cols] = narrow(dot(both, jnp.concatenate([part, part], axis=0)))
            copies.append(
                pltpu.make_async_copy(
                    stage.at[k, :, cols], outs[k].at[:, cols], sems.at[k * chunks + j]
                )
            )
            copies[-1].start()
    if graded:
        dots, ids = refs[3], refs[4]
        slots = slot_rows(ids[...], pad)
        found = jnp.sum(slots * dots[...], axis=0, keepdims=True)
        refs[7][...] = jnp.where(ids[...] == 0, found, 0.0)
    for copy in copies:
        copy.wait()


def mix(block_f, block_b, tables, rows, grading):
    block_rows, width = block_f.shape
    tokens = tables.shape[1]
    chunks = block_rows // rows
    vmem = pl.BlockSpec(memory_space=pltpu.VMEM)
    anywhere = pl.BlockSpec(memory_space=pl.ANY)
    shape = jax.ShapeDtypeStruct((tokens, chunks * width), jnp.bfloat16)
    out_shape = [shape, shape]
    if grading:
        out_shape.append(jax.ShapeDtypeStruct(grading[1].shape, jnp.float32))
    return pl.pallas_call(
        functools.partial(mix_kernel, rows, bool(grading)),
        out_shape=tuple(out_shape),
        in_specs=[vmem] * (3 + len(grading)),
        out_specs=tuple([anywhere, anywhere] + [vmem] * (len(out_shape) - 2)),
        scratch_shapes=[
            pltpu.VMEM((2, tokens, chunks * width), jnp.bfloat16),
            pltpu.SemaphoreType.DMA((2 * chunks,)),
        ],
        name="mix",
    )(block_f, block_b, tables, *grading)


def body(
    act_in,
    cotangent,
    fwd_ids,
    fwd_gates,
    bwd_ids,
    bwd_gates,
    gate_w,
    up_w,
    down_w,
    gate_pre,
    up_pre,
):
    ndev = lax.axis_size("expert")
    ff_dev = gate_w.shape[2]
    slices = FF // ff_dev
    experts = ndev // slices
    capacity = gate_pre.shape[1] // ndev
    rows = experts * capacity
    weights = (gate_w[0], up_w[0], down_w[0])

    if experts == 1:
        routes = tuple(each[0].T for each in (fwd_ids, fwd_gates, bwd_ids, bwd_gates))
        block_f, block_b, dots, tables = run_layer(
            act_in[0], cotangent[0], *weights, gate_pre[0], up_pre[0], routes, slices, rows
        )
        next_act, prev_grad, grads = mix(block_f, block_b, tables, rows, (dots, routes[2]))
        return (next_act[None], prev_grad[None], grads.T[None])

    chunks = 16 // math.gcd(16, rows)
    features = act_in.shape[2]
    width = features // chunks
    columns = [[g * slices + i for g in range(experts)] for i in range(slices)]

    def exchange(value):
        return lax.all_to_all(
            value, "expert", split_axis=0, concat_axis=0, axis_index_groups=columns, tiled=True
        )

    matches_f, placing_f, weights_f = routing(fwd_ids[0], fwd_gates[0], experts, capacity)
    matches_b, placing_b, weights_b = routing(bwd_ids[0], bwd_gates[0], experts, capacity)

    def prepare(tokens, placing):
        chosen = placing.reshape(rows, tokens.shape[0])
        picked = dot(chosen.astype(jnp.bfloat16), tokens).astype(jnp.bfloat16)
        picked = exchange(picked.reshape(experts, capacity, features))
        return picked.reshape(rows, features)

    def by_group(saved):
        saved = saved.reshape(experts, slices, capacity, ff_dev).transpose(1, 0, 2, 3)
        return saved.reshape(slices * rows, ff_dev)

    block_f, block_b, dots = run_layer(
        prepare(act_in[0], placing_f), prepare(cotangent[0], placing_b), *weights,
        by_group(gate_pre[0]), by_group(up_pre[0]), (), slices, rows,
    )
    mine = exchange(dots[:rows, 0].reshape(experts, capacity))

    def send_back(block):
        table = block.reshape(chunks, rows, width).transpose(1, 0, 2)
        table = exchange(table.reshape(experts, capacity, features))
        table = table.reshape(rows, chunks, width).transpose(1, 0, 2)
        return table.reshape(chunks * rows, width)

    token_dots = jnp.sum(placing_b * mine[:, :, None], axis=1)
    gate_grad = jnp.sum(jnp.where(matches_b, token_dots[:, :, None], 0.0), axis=0)

    def weight_table(placing, weights):
        table = (placing * weights[:, None, :]).reshape(rows, -1).T
        return jnp.pad(table, ((0, 0), (0, LANES - rows)))

    def onward(block, placing, weights, step):
        block = from_behind(send_back(block), "section", step)
        return block, from_behind(weight_table(placing, weights), "section", step)

    block_f, table_f = onward(block_f, placing_f, weights_f, 1)
    block_b, table_b = onward(block_b, placing_b, weights_b, -1)
    next_act, prev_grad = mix(block_f, block_b, jnp.stack([table_f, table_b]), rows, ())
    return (next_act[None], prev_grad[None], gate_grad[None])


def solution(mesh):
    in_specs = (
        P("section", "expert", None),
        P("section", "expert", None),
        P("section", "expert", None),
        P("section", "expert", None),
        P("section", "expert", None),
        P("section", "expert", None),
        P("section", None, "expert"),
        P("section", None, "expert"),
        P("section", "expert", None),
        P("section", None, "expert"),
        P("section", None, "expert"),
    )
    out_specs = (
        P("section", "expert", None),
        P("section", "expert", None),
        P("section", "expert", None),
    )
    return jax.shard_map(body, mesh=mesh, in_specs=in_specs, out_specs=out_specs, check_vma=False)
```

```python
import functools
import math

import jax
import jax.numpy as jnp
from jax import lax
from jax.experimental import pallas as pl
from jax.experimental.pallas import tpu as pltpu
from jax.sharding import PartitionSpec as P

FF = 2048
QUAD = 4
LANES = 128
SEMAPHORES = 192
SPLIT = (1, 2)
TABLES_AFTER = "fwd 0 B"
MESH = pl.DeviceIdType.MESH

SCHEDULE = (
    "place 0", "ox 0 0", "oy 0 0", "zs 0 1", "place 1", "oy 1 B", "oy 0 B", "ox 1 0", "zs 1 1",
    "oy 1 0", "ox 1 B", "ox 0 B", "zs 0 2", "ox 0 1", "oy 0 1", "fwd 1 B", "fwd 0 0", "zs 1 2",
    "oy 1 1", "fwd 0 B", "zs 0 3", "ox 1 1", "oy 0 2", "zs 1 3", "ox 1 2", "zB 1 1", "oy 1 2",
    "zB 0 1", "oy 0 3", "ox 0 3", "ox 1 3", "fwd 1 1", "comp 0 0", "ox 0 2", "fwd 1 2",
    "oy 1 3", "fwd 0 2", "zB 1 2", "fwd 0 1", "zB 0 2", "fwd 0 3", "comp 1 1", "zB 1 3",
    "fwd 1 3", "rf 1 1", "comp 1 2", "rb 1 2", "zB 0 3", "rf 1 2", "rn 1 1", "comp 0 2",
    "rn 1 2", "rb 0 2", "rb 1 1", "fwd 1 0", "rf 0 2", "rn 0 2", "comp 1 3", "sec 1 2",
    "rb 1 3", "sec 1 1", "comp 0 3", "rf 0 3", "rb 0 3", "comp 0 1", "rf 0 1", "sec 0 2",
    "rf 1 3", "rb 0 1", "rn 0 3", "thi 1 2", "rz 1 2", "sec 0 3", "thi 0 2", "sumB 0", "rn 0 1",
    "thi 1 1", "rz 0 2", "rz 1 1", "rn 1 3", "sec 0 1", "comp 1 0", "sec 1 3", "sumB 1",
    "thi 0 3", "rf 0 0", "rz 0 3", "rn 0 0", "rf 1 0", "sec 0 B", "thi 1 3", "rz 1 3",
    "thi 0 1", "rn 1 0", "sec 1 B", "rz 0 1", "sec 0 0", "sec 1 0", "thi 1 B", "thi 0 B",
    "thi 0 0", "fin 0", "thi 1 0", "fin 1", "del 0", "del 1",
)
GATHER_X = (
    {"B": False, 0: True, 1: True, 2: True, 3: False},
    {"B": True, 0: True, 1: False, 2: False, 3: False},
)
REDUCE_X = (
    {"B": False, 0: True, 1: False, 2: False, 3: True},
    {"B": False, 0: False, 1: True, 2: False, 3: True},
)


def from_behind(value, axis, steps):
    count = lax.axis_size(axis)
    pairs = [(source, (source + steps) % count) for source in range(count)]
    return lax.ppermute(value, axis, pairs)


def routing(ids, gates, experts, capacity):
    expert_ids = jnp.arange(experts, dtype=jnp.int32)
    matches = ids[None, :, :] == expert_ids[:, None, None]
    routed = jnp.any(matches, axis=2)
    weights = jnp.sum(jnp.where(matches, gates[None, :, :], 0.0), axis=2)
    tokens = ids.shape[0]
    earlier = jnp.arange(tokens)[:, None] <= jnp.arange(tokens)[None, :]
    counted = jnp.sum(jnp.where(routed[:, :, None] & earlier[None], 1, 0), axis=1)
    position = counted - 1
    slot_ids = jnp.arange(capacity, dtype=jnp.int32)
    placing = (position[:, None, :] == slot_ids[None, :, None]) & routed[:, None, :]
    return (matches, placing.astype(jnp.float32), weights)


def xor(value, mask):
    out = value
    bit = 1
    while bit <= mask:
        if mask & bit:
            out = out + bit - 2 * bit * ((value // bit) % 2)
        bit *= 2
    return out


def dot(a, b, dims=((1,), (0,))):
    return lax.dot_general(a, b, (dims, ((), ())), preferred_element_type=jnp.float32)


def wide(value):
    return value.astype(jnp.float32)


def narrow(value):
    return value.astype(jnp.bfloat16)


def padded(rows):
    return -(-rows // 16) * 16


def selection(count, rows, pad, flip=False):
    shape = (count * rows, count * pad) if flip else (count * pad, count * rows)
    long = lax.broadcasted_iota(jnp.int32, shape, 1 if flip else 0)
    short = lax.broadcasted_iota(jnp.int32, shape, 0 if flip else 1)
    piece = lax.shift_right_logical(long, jnp.int32(pad.bit_length() - 1))
    inner = long & (pad - 1)
    chosen = (short == piece * rows + inner) & (inner < rows)
    return narrow(jnp.where(chosen, 1.0, 0.0))


def slot_rows(ids, count):
    tokens = ids.shape[1]
    routed = jnp.max(jnp.where(ids == 0, 1.0, 0.0), axis=0, keepdims=True)
    spread = jnp.broadcast_to(routed, (count, tokens))
    row = lax.broadcasted_iota(jnp.int32, (tokens, tokens), 0)
    column = lax.broadcasted_iota(jnp.int32, (tokens, tokens), 1)
    upper = narrow(jnp.where(row <= column, 1.0, 0.0))
    rank = dot(narrow(spread), upper) - 1.0
    slot = wide(lax.broadcasted_iota(jnp.int32, (count, tokens), 0))
    return jnp.where((rank == slot) & (spread > 0.0), 1.0, 0.0)


class Links:
    def __init__(self, send_sems, recv_sems):
        self.send_sems = send_sems
        self.recv_sems = recv_sems
        self.count = 0
        self.sent = []

    def copy(self, src, dst, peer, axis="expert"):
        k = self.count
        self.count += 1
        assert k < SEMAPHORES
        return pltpu.make_async_remote_copy(
            src_ref=src,
            dst_ref=dst,
            send_sem=self.send_sems.at[k],
            recv_sem=self.recv_sems.at[k],
            device_id={axis: peer},
            device_id_type=MESH,
        )

    def start(self, copy):
        copy.start()
        self.sent.append(copy)


def layer_kernel(slices, chunks, rows, hop, *refs):
    inputs = 11 if hop else 7
    tok_f, tok_b, w_gate, w_up, w_down, pre_gate, pre_up = refs[:7]
    routes = refs[7:inputs]
    outs = 4 if hop else 3
    out_f, out_b, out_dots = refs[inputs : inputs + 3]
    (
        tok, wc, wd, gat_a0, gat_b0, gat_a1, gat_b1, par_a, par_b, xb, yb, pre, rs1, rs2, rsz, hold, hold2, zgot_b,
        sum_b, rs1_b, rs2_b, hold_b, sums, landed, table, table_got, dot_out, dot_in, ids_got, gates_got, pre_got, local_sems,
        send_sems, recv_sems,
    ) = refs[inputs + outs :]
    device = lax.axis_index("expert")
    me = device % slices
    base = device - me
    lo = me % QUAD
    z = me // QUAD
    depth = slices // QUAD
    xp = base + xor(me, 1)
    yp = base + xor(me, 2)
    zp = [base + xor(z, q) * QUAD + lo for q in range(depth)]
    features, ff = wc.shape[0], wd.shape[0]
    width = features // chunks
    pad = padded(rows)
    gat_a, gat_b = (gat_a0, gat_a1), (gat_b0, gat_b1)
    cut = par_a.shape[3]

    def bid(q, mask):
        return xor(z, q) * QUAD + xor(lo, mask)

    def cols_of(j):
        return pl.ds(j * width, width)

    loads = []

    def load(src, dst):
        copy = pltpu.make_async_copy(src, dst, local_sems.at[len(loads)])
        loads.append(copy)
        copy.start()
        return copy

    load_route = []
    for k in range(len(routes)):
        load_route.append(load(routes[k], (gates_got if k % 2 else ids_got).at[k // 2]))
    load_f = [load(tok_f.at[:, cols_of(j)], tok.at[0, :, cols_of(j)]) for j in range(chunks)]

    barrier = pltpu.get_barrier_semaphore()
    peers = [(q, m) for q in range(depth) for m in range(QUAD) if q or m]
    for q, m in peers:
        pl.semaphore_signal(
            barrier, inc=1, device_id={"expert": base + bid(q, m)}, device_id_type=MESH
        )
    greeted = len(peers)
    if hop:
        section = lax.axis_index("section")
        sections = lax.axis_size("section")
        ahead = (section + 1) % sections
        behind = (section + sections - 1) % sections
        for peer in (ahead, behind):
            pl.semaphore_signal(barrier, inc=1, device_id={"section": peer}, device_id_type=MESH)
        greeted += 2

    load_b, load_w = [], []

    def start_loads():
        for j in range(chunks):
            load_b.append(load(tok_b.at[:, cols_of(j)], tok.at[1, :, cols_of(j)]))
        for j in range(chunks):
            load_w.append(load(w_gate.at[cols_of(j), :], wc.at[cols_of(j), pl.ds(0, ff)]))
            load_w.append(load(w_up.at[cols_of(j), :], wc.at[cols_of(j), pl.ds(ff, ff)]))
            load_w.append(load(w_down.at[:, cols_of(j)], wd.at[:, cols_of(j)]))
        load_w.append(load(pre_gate, pre_got.at[0]))
        load_w.append(load(pre_up, pre_got.at[1]))

    unpack = selection(chunks, rows, pad)
    pack = selection(chunks, rows, pad, flip=True)

    def choose(mb):
        if not hop:
            shape = (pad, tok.shape[1])
            same = lax.broadcasted_iota(jnp.int32, shape, 0)
            return narrow(
                jnp.where(same == lax.broadcasted_iota(jnp.int32, shape, 1), 1.0, 0.0)
            )
        load_route[2 * mb].wait()
        return narrow(slot_rows(ids_got[mb], pad))

    def send_tables():
        for mb in range(2):
            load_route[2 * mb + 1].wait()
            ids = ids_got[mb]
            gates = jnp.where(ids == 0, gates_got[mb], 0.0)
            weighted = slot_rows(ids, LANES) * jnp.sum(gates, axis=0, keepdims=True)
            table[mb] = jnp.transpose(weighted)
            links.start(tables[mb])

    def place(mb, chosen, waits):
        for j in range(chunks):
            waits[j].wait()
            if mb == 0 and j == chunks - 1:
                start_loads()
            picked = dot(chosen, tok[mb, :, cols_of(j)])
            yb[0, pl.ds(j * pad, pad), :] = narrow(picked)
        packed = narrow(dot(pack, yb[0]))
        edge = gat_a[mb].shape[2]
        gat_a[mb][me] = packed[:, :edge]
        gat_b[mb][me] = packed[:, edge:]

    links = Links(send_sems, recv_sems)
    offsets = range(1, depth)
    own_x, own_y, forward, r1, r2 = {}, {}, {}, {}, {}
    zsend, rz, bsend, rb, dots_sent = {}, {}, {}, {}, {}
    for mb in range(2):
        for q in offsets:
            rz[mb, q] = links.copy(hold2.at[mb, q], rsz.at[mb, q], zp[q])
            for up in (1, -1):
                source = jnp.clip(z - up * (q - 1), 0, depth - 1)
                peer = base + jnp.clip(z + up, 0, depth - 1) * QUAD + lo
                block = gat_a[mb].at[source * QUAD + lo]
                zsend[mb, q, up] = links.copy(block, block, peer)
                quad = gat_b[mb].at[pl.ds(source * QUAD, QUAD)]
                bsend[mb, q, up] = links.copy(quad, quad, peer)
            theirs = par_b.at[mb, pl.ds(xor(z, q) * QUAD, QUAD)]
            rb[mb, q] = links.copy(theirs, zgot_b.at[mb, q], zp[q])
        for step in ["B"] + list(range(depth)):
            at = (mb, step)
            q, gat = (0, gat_b[mb]) if step == "B" else (step, gat_a[mb])
            block = gat.at[bid(q, 0)]
            own_x[at] = links.copy(block, block, xp)
            own_y[at] = links.copy(block, block, yp)
            via_x = GATHER_X[mb][step]
            got = gat.at[bid(q, 2 if via_x else 1)]
            forward[at] = links.copy(got, got, xp if via_x else yp)
            m1, p1, p2 = (1, xp, yp) if REDUCE_X[mb][step] else (2, yp, xp)
            if step == "B":
                far, near = sum_b.at[mb, xor(lo, 3)], sum_b.at[mb, xor(lo, m1)]
                got1, held, got2 = rs1_b.at[mb], hold_b.at[mb], rs2_b.at[mb]
            else:
                far, near = par_a.at[mb, bid(q, 3)], par_a.at[mb, bid(q, m1)]
                got1, held, got2 = rs1.at[mb, q], hold.at[mb, q], rs2.at[mb, q]
            r1[at] = [links.copy(far, got1.at[1], p1), links.copy(near, got1.at[0], p1)]
            r2[at] = links.copy(held, got2, p2)
    for q in range(depth):
        dots_sent[q] = [
            links.copy(dot_out.at[bid(q, m)], dot_in.at[q * QUAD + m], base + bid(q, m))
            for m in range(QUAD)
            if q or m
        ]
    if hop:
        across = [
            links.copy(sums.at[0], landed.at[0], ahead, "section"),
            links.copy(sums.at[1], landed.at[1], behind, "section"),
        ]
        tables = [
            links.copy(table.at[0], table_got.at[0], ahead, "section"),
            links.copy(table.at[1], table_got.at[1], behind, "section"),
        ]

    arrived = []

    def await_all(*copies):
        for copy in copies:
            if not any(copy is done for done in arrived):
                arrived.append(copy)
                copy.wait_recv()

    def do_place(mb):
        place(mb, choose(mb), load_b if mb else load_f)
        if mb == 0:
            pl.semaphore_wait(barrier, greeted)

    def chain(sends, mb, hop):
        for up in (1, -1):
            source, onward = z - up * (hop - 1), z + up
            held = (source >= 0) & (source < depth)
            if hop > 1:

                @pl.when(held)
                def _():
                    sends[mb, hop - 1, up].wait_recv()

            @pl.when(held & (onward >= 0) & (onward < depth))
            def _():
                sends[mb, hop, up].start()

    ended = []

    def last_hop(sends, mb):
        if (sends is bsend, mb) not in ended:
            ended.append((sends is bsend, mb))
            for up in (1, -1):
                source = z - up * (depth - 1)

                @pl.when((source >= 0) & (source < depth))
                def _():
                    sends[mb, depth - 1, up].wait_recv()

    def finish_chain(sends, mb):
        for hop in range(1, depth):
            for up in (1, -1):
                source, onward = z - up * (hop - 1), z + up
                held = (source >= 0) & (source < depth)

                @pl.when(held & (onward >= 0) & (onward < depth))
                def _():
                    sends[mb, hop, up].wait_send()

    def do_zs(mb, hop):
        chain(zsend, mb, hop)

    def do_own(mb, step, copies):
        if step == depth - 1:
            last_hop(zsend, mb)
        links.start(copies[mb, step])

    def do_fwd(mb, step):
        await_all((own_y if GATHER_X[mb][step] else own_x)[mb, step])
        links.start(forward[mb, step])

    def await_quad(mb, step):
        await_all(own_x[mb, step], own_y[mb, step], forward[mb, step])

    def do_bsend(mb, hop):
        if hop == 1:
            await_quad(mb, "B")
        chain(bsend, mb, hop)

    ready = []

    def do_compute(mb, q):
        await_quad(mb, q)
        if q == 0:
            await_quad(mb, "B")
        elif q == depth - 1:
            last_hop(bsend, mb)
        if not ready:
            ready.append(True)
            for copy in load_w:
                copy.wait()
            spaced = selection(slices, rows, pad)
            for k in range(2):
                pre[k] = narrow(dot(spaced, pre_got[k])).reshape(pre.shape[1:])
        zq = xor(z, q)
        group = zq * QUAD
        for b in range(QUAD):
            full_a = narrow(dot(unpack, gat_a[mb][group + b]))
            full_b = narrow(dot(unpack, gat_b[mb][group + b]))
            edge = full_a.shape[1]
            for j in range(chunks):
                piece_rows = slice(j * pad, (j + 1) * pad)
                xb[pl.ds(b * pad, pad), pl.ds(j * width, edge)] = full_a[piece_rows]
                after = pl.ds(j * width + edge, width - edge)
                xb[pl.ds(b * pad, pad), after] = full_b[piece_rows]
        total = None
        for j in range(chunks):
            if mb == 0:
                part = dot(xb[:, cols_of(j)], wc[cols_of(j), :])
            else:
                part = dot(xb[:, cols_of(j)], wd[:, cols_of(j)], ((1,), (1,)))
            total = part if total is None else total + part
        if mb == 0:
            gate = total[:, :ff]
            hidden = narrow(gate / (1.0 + jnp.exp(-gate)) * total[:, ff:])

            def piece(j):
                return dot(hidden, wd[:, cols_of(j)])

        else:
            gate = wide(pre[0, zq])
            up = wide(pre[1, zq])
            sig = 1.0 / (1.0 + jnp.exp(-gate))
            activated = gate * sig
            dots = jnp.sum(total * activated * up, axis=1, keepdims=True)
            for b in range(QUAD):
                mine = dots[b * pad : (b + 1) * pad]
                dot_out[group + b] = jnp.broadcast_to(mine, (pad, LANES))
            grad_gate = narrow(total * up * sig * (1.0 + gate * (1.0 - sig)))
            both = jnp.concatenate([grad_gate, narrow(total * activated)], axis=1)

            def piece(j):
                return dot(both, wc[cols_of(j), :], ((1,), (1,)))

        for j in range(chunks):
            full = narrow(piece(j))
            for b in range(QUAD):
                yb[b, pl.ds(j * pad, pad), :] = full[b * pad : (b + 1) * pad]
        for b in range(QUAD):
            packed = narrow(dot(pack, yb[b]))
            par_a[mb, group + b] = packed[:, :cut]
            par_b[mb, group + b] = packed[:, cut:]
        if mb == 1:
            for copy in dots_sent[q]:
                links.start(copy)

    def do_gather_b(mb):
        total = wide(par_b[mb, pl.ds(z * QUAD, QUAD)])
        for q in offsets:
            await_all(rb[mb, q])
            total = total + wide(zgot_b[mb, q])
        sum_b[mb] = narrow(total)
        for copy in r1[mb, "B"]:
            links.start(copy)

    def shares(mb, step):
        if step == "B":
            return (lambda m: sum_b[mb, xor(lo, m)]), rs1_b.at[mb], hold_b.at[mb], rs2_b.at[mb]
        q = step
        return (lambda m: par_a[mb, bid(q, m)]), rs1.at[mb, q], hold.at[mb, q], rs2.at[mb, q]

    def do_second(mb, step):
        mine, got, held, unused = shares(mb, step)
        await_all(r1[mb, step][0])
        held[...] = narrow(wide(mine(2 if REDUCE_X[mb][step] else 1)) + wide(got[1]))
        links.start(r2[mb, step])

    def do_third(mb, step):
        mine, got, unused, got2 = shares(mb, step)
        await_all(r1[mb, step][1], r2[mb, step])
        total = narrow(wide(mine(0)) + wide(got[0]) + wide(got2[...]))
        if step == "B":
            sums[mb, :, pl.ds(cut, width - cut)] = total
        else:
            hold2[mb, step] = total

    def do_finish(mb):
        total = wide(hold2[mb, 0])
        for q in offsets:
            await_all(rz[mb, q])
            total = total + wide(rsz[mb, q])
        sums[mb, :, pl.ds(0, cut)] = narrow(total)
        if hop:
            links.start(across[mb])

    def do_deliver(mb):
        out = (out_f, out_b)[mb]
        if mb == 1:
            found = dot_out[me]
            for q, m in peers:
                copy = links_to[q, m]
                await_all(copy)
                found = found + dot_in[q * QUAD + m]
            out_dots[...] = found
            if hop:
                out_tables = refs[inputs + 3]
                await_all(*tables)
                out_tables[...] = table_got[...]
        if hop:
            await_all(across[mb])
            out[...] = landed[mb]
        else:
            out[...] = sums[mb]

    links_to = {}
    for q in range(depth):
        masks = [m for m in range(QUAD) if q or m]
        for m, copy in zip(masks, dots_sent[q]):
            links_to[q, m] = copy

    events = {
        "place": do_place,
        "zs": do_zs,
        "ox": lambda mb, step: do_own(mb, step, own_x),
        "oy": lambda mb, step: do_own(mb, step, own_y),
        "fwd": do_fwd,
        "zB": do_bsend,
        "comp": do_compute,
        "rb": lambda mb, q: links.start(rb[mb, q]),
        "rf": lambda mb, q: links.start(r1[mb, q][0]),
        "rn": lambda mb, q: links.start(r1[mb, q][1]),
        "rz": lambda mb, q: links.start(rz[mb, q]),
        "sumB": do_gather_b,
        "sec": do_second,
        "thi": do_third,
        "fin": do_finish,
        "del": do_deliver,
    }
    for entry in SCHEDULE:
        event, *at = entry.split()
        events[event](*(step if step == "B" else int(step) for step in at))
        if entry == TABLES_AFTER and hop:
            send_tables()
    for mb in range(2):
        finish_chain(zsend, mb)
        finish_chain(bsend, mb)
    for copy in links.sent:
        copy.wait_send()


def run_layer(tok_f, tok_b, w_gate, w_up, w_down, pre_gate, pre_up, routes, slices, rows):
    hop = bool(routes)
    features = tok_f.shape[1]
    chunks = 16 // math.gcd(16, rows)
    width = features // chunks
    ff = w_gate.shape[1]
    depth = slices // QUAD
    pad = padded(rows)
    group = QUAD * pad

    vmem = pl.BlockSpec(memory_space=pltpu.VMEM)
    anywhere = pl.BlockSpec(memory_space=pltpu.HBM)
    block = (chunks * rows, width)
    last = max(width // LANES // 7, 1) * LANES
    gathers = []
    for sevenths in SPLIT:
        for columns in (width - sevenths * last, sevenths * last):
            gathers.append(pltpu.VMEM((slices, chunks * rows, columns), jnp.bfloat16))
    part_a, part_b = (chunks * rows, width - last), (chunks * rows, last)
    tables = (2, tok_f.shape[0] if hop else 8, LANES)
    choices = routes[0].shape if hop else (8, LANES)
    out_shape = [
        jax.ShapeDtypeStruct(block, jnp.bfloat16),
        jax.ShapeDtypeStruct(block, jnp.bfloat16),
        jax.ShapeDtypeStruct((pad, LANES), jnp.float32),
    ]
    if hop:
        out_shape.append(jax.ShapeDtypeStruct(tables, jnp.float32))
    return pl.pallas_call(
        functools.partial(layer_kernel, slices, chunks, rows, hop),
        out_shape=tuple(out_shape),
        in_specs=[anywhere] * (7 + len(routes)),
        out_specs=(vmem,) * len(out_shape),
        scratch_shapes=[
            pltpu.VMEM((2,) + tok_f.shape, jnp.bfloat16),
            pltpu.VMEM((features, 2 * ff), jnp.bfloat16),
            pltpu.VMEM((ff, features), jnp.bfloat16),
            *gathers,
            pltpu.VMEM((2, slices) + part_a, jnp.bfloat16),
            pltpu.VMEM((2, slices) + part_b, jnp.bfloat16),
            pltpu.VMEM((group, features), jnp.bfloat16),
            pltpu.VMEM((QUAD, chunks * pad, width), jnp.bfloat16),
            pltpu.VMEM((2, depth, group, ff), jnp.bfloat16),
            pltpu.VMEM((2, depth, 2) + part_a, jnp.bfloat16),
            pltpu.VMEM((2, depth) + part_a, jnp.bfloat16),
            pltpu.VMEM((2, depth) + part_a, jnp.bfloat16),
            pltpu.VMEM((2, depth) + part_a, jnp.bfloat16),
            pltpu.VMEM((2, depth) + part_a, jnp.bfloat16),
            pltpu.VMEM((2, depth, QUAD) + part_b, jnp.bfloat16),
            pltpu.VMEM((2, QUAD) + part_b, jnp.bfloat16),
            pltpu.VMEM((2, 2) + part_b, jnp.bfloat16),
            pltpu.VMEM((2,) + part_b, jnp.bfloat16),
            pltpu.VMEM((2,) + part_b, jnp.bfloat16),
            pltpu.VMEM((2,) + block, jnp.bfloat16),
            pltpu.VMEM((2,) + block, jnp.bfloat16),
            pltpu.VMEM(tables, jnp.float32),
            pltpu.VMEM(tables, jnp.float32),
            pltpu.VMEM((slices, pad, LANES), jnp.float32),
            pltpu.VMEM((slices, pad, LANES), jnp.float32),
            pltpu.VMEM((2,) + choices, jnp.int32),
            pltpu.VMEM((2,) + choices, jnp.float32),
            pltpu.VMEM((2,) + pre_gate.shape, jnp.bfloat16),
            pltpu.SemaphoreType.DMA((5 * chunks + 6,)),
            pltpu.SemaphoreType.DMA((SEMAPHORES,)),
            pltpu.SemaphoreType.DMA((SEMAPHORES,)),
        ],
        compiler_params=pltpu.CompilerParams(
            collective_id=0, has_side_effects=True, vmem_limit_bytes=56 * 2**20
        ),
        name="moe_layer",
    )(tok_f, tok_b, w_gate, w_up, w_down, pre_gate, pre_up, *routes)


def mix_kernel(rows, graded, *refs):
    block_f, block_b, tables = refs[:3]
    extra = 2 if graded else 0
    outs = refs[3 + extra : 5 + extra]
    stage, sems = refs[-2:]
    block_rows, width = block_f.shape
    chunks = block_rows // rows
    pad = padded(rows)
    unpack = selection(chunks, rows, pad)
    copies = []
    for k, block in enumerate((block_f, block_b)):
        weight = tables[k][:, :pad]
        high = narrow(weight)
        both = jnp.concatenate([high, narrow(weight - wide(high))], axis=1)
        full = narrow(dot(unpack, block[...]))
        for j in range(chunks):
            part = full[j * pad : (j + 1) * pad]
            cols = pl.ds(j * width, width)
            stage[k, :, cols] = narrow(dot(both, jnp.concatenate([part, part], axis=0)))
            copies.append(
                pltpu.make_async_copy(
                    stage.at[k, :, cols], outs[k].at[:, cols], sems.at[k * chunks + j]
                )
            )
            copies[-1].start()
    if graded:
        dots, ids = refs[3], refs[4]
        slots = slot_rows(ids[...], pad)
        found = jnp.sum(slots * dots[...], axis=0, keepdims=True)
        refs[7][...] = jnp.where(ids[...] == 0, found, 0.0)
    for copy in copies:
        copy.wait()


def mix(block_f, block_b, tables, rows, grading):
    block_rows, width = block_f.shape
    tokens = tables.shape[1]
    chunks = block_rows // rows
    vmem = pl.BlockSpec(memory_space=pltpu.VMEM)
    anywhere = pl.BlockSpec(memory_space=pl.ANY)
    shape = jax.ShapeDtypeStruct((tokens, chunks * width), jnp.bfloat16)
    out_shape = [shape, shape]
    if grading:
        out_shape.append(jax.ShapeDtypeStruct(grading[1].shape, jnp.float32))
    return pl.pallas_call(
        functools.partial(mix_kernel, rows, bool(grading)),
        out_shape=tuple(out_shape),
        in_specs=[vmem] * (3 + len(grading)),
        out_specs=tuple([anywhere, anywhere] + [vmem] * (len(out_shape) - 2)),
        scratch_shapes=[
            pltpu.VMEM((2, tokens, chunks * width), jnp.bfloat16),
            pltpu.SemaphoreType.DMA((2 * chunks,)),
        ],

        name="mix",
    )(block_f, block_b, tables, *grading)


def body(
    act_in,
    cotangent,
    fwd_ids,
    fwd_gates,
    bwd_ids,
    bwd_gates,
    gate_w,
    up_w,
    down_w,
    gate_pre,
    up_pre,
):
    ndev = lax.axis_size("expert")
    ff_dev = gate_w.shape[2]
    slices = FF // ff_dev
    experts = ndev // slices
    capacity = gate_pre.shape[1] // ndev
    rows = experts * capacity
    weights = (gate_w[0], up_w[0], down_w[0])

    if experts == 1:
        routes = tuple(each[0].T for each in (fwd_ids, fwd_gates, bwd_ids, bwd_gates))
        block_f, block_b, dots, tables = run_layer(
            act_in[0], cotangent[0], *weights, gate_pre[0], up_pre[0], routes, slices, rows
        )
        next_act, prev_grad, grads = mix(block_f, block_b, tables, rows, (dots, routes[2]))
        return (next_act[None], prev_grad[None], grads.T[None])

    chunks = 16 // math.gcd(16, rows)
    features = act_in.shape[2]
    width = features // chunks
    columns = [[g * slices + i for g in range(experts)] for i in range(slices)]

    def exchange(value):
        return lax.all_to_all(
            value, "expert", split_axis=0, concat_axis=0, axis_index_groups=columns, tiled=True
        )

    matches_f, placing_f, weights_f = routing(fwd_ids[0], fwd_gates[0], experts, capacity)
    matches_b, placing_b, weights_b = routing(bwd_ids[0], bwd_gates[0], experts, capacity)

    def prepare(tokens, placing):
        chosen = placing.reshape(rows, tokens.shape[0])
        picked = dot(chosen.astype(jnp.bfloat16), tokens).astype(jnp.bfloat16)
        picked = exchange(picked.reshape(experts, capacity, features))
        return picked.reshape(rows, features)

    def by_group(saved):
        saved = saved.reshape(experts, slices, capacity, ff_dev).transpose(1, 0, 2, 3)
        return saved.reshape(slices * rows, ff_dev)

    block_f, block_b, dots = run_layer(
        prepare(act_in[0], placing_f), prepare(cotangent[0], placing_b), *weights,
        by_group(gate_pre[0]), by_group(up_pre[0]), (), slices, rows,
    )
    mine = exchange(dots[:rows, 0].reshape(experts, capacity))

    def send_back(block):
        table = block.reshape(chunks, rows, width).transpose(1, 0, 2)
        table = exchange(table.reshape(experts, capacity, features))
        table = table.reshape(rows, chunks, width).transpose(1, 0, 2)
        return table.reshape(chunks * rows, width)

    token_dots = jnp.sum(placing_b * mine[:, :, None], axis=1)
    gate_grad = jnp.sum(jnp.where(matches_b, token_dots[:, :, None], 0.0), axis=0)

    def weight_table(placing, weights):
        table = (placing * weights[:, None, :]).reshape(rows, -1).T
        return jnp.pad(table, ((0, 0), (0, LANES - rows)))

    def onward(block, placing, weights, step):
        block = from_behind(send_back(block), "section", step)
        return block, from_behind(weight_table(placing, weights), "section", step)

    block_f, table_f = onward(block_f, placing_f, weights_f, 1)
    block_b, table_b = onward(block_b, placing_b, weights_b, -1)
    next_act, prev_grad = mix(block_f, block_b, jnp.stack([table_f, table_b]), rows, ())
    return (next_act[None], prev_grad[None], gate_grad[None])


def solution(mesh):
    in_specs = (
        P("section", "expert", None),
        P("section", "expert", None),
        P("section", "expert", None),
        P("section", "expert", None),
        P("section", "expert", None),
        P("section", "expert", None),
        P("section", None, "expert"),
        P("section", None, "expert"),
        P("section", "expert", None),
        P("section", None, "expert"),
        P("section", None, "expert"),
    )
    out_specs = (
        P("section", "expert", None),
        P("section", "expert", None),
        P("section", "expert", None),
    )
    return jax.shard_map(body, mesh=mesh, in_specs=in_specs, out_specs=out_specs, check_vma=False)
```
